32 devices in a mesh: dp: 4 (over y, z), tp: 8 (over x, core).
Axes of the slice: x: 4, y: 2, z: 2, core: 2. Of those that a mesh axis runs over, the one named last changes fastest.
The devices are a block of a 4x4x8 slice.
Arguments:
- hidden: bfloat16 [8, 3840], P('dp'), parts along dimension 0
- positions: int32 [8], P('dp'), parts along dimension 0
- k_local: bfloat16 [8, 1024, 8, 256], P('dp', None, 'tp'), parts along dimension 0
- v_local: bfloat16 [8, 1024, 8, 256], P('dp', None, 'tp'), parts along dimension 0
- k_global: bfloat16 [8, 4096, 8, 256], P('dp', None, 'tp'), parts along dimension 0
- v_global: bfloat16 [8, 4096, 8, 256], P('dp', None, 'tp'), parts along dimension 0
- w_query: bfloat16 [2, 3840, 4096], P(None, None, 'tp')
- w_key: bfloat16 [2, 3840, 2048], P(None, None, 'tp')
- w_value: bfloat16 [2, 3840, 2048], P(None, None, 'tp')
- w_out: bfloat16 [2, 4096, 3840], P(None, 'tp')
- w_gate: bfloat16 [2, 3840, 15360], P(None, None, 'tp')
- w_up: bfloat16 [2, 3840, 15360], P(None, None, 'tp')
- w_down: bfloat16 [2, 15360, 3840], P(None, 'tp')
- norm_scale: float32 [2, 4, 3840], replicated
Outputs:
- output 1: bfloat16 [8, 3840], P('dp'), parts along dimension 0
- output 2: bfloat16 [8, 1024, 8, 256], P('dp', None, 'tp'), parts along dimension 0
- output 3: bfloat16 [8, 1024, 8, 256], P('dp', None, 'tp'), parts along dimension 0
- output 4: bfloat16 [8, 4096, 8, 256], P('dp', None, 'tp'), parts along dimension 0
- output 5: bfloat16 [8, 4096, 8, 256], P('dp', None, 'tp'), parts along dimension 0
There are 4 independent parts. The reference program is written for one: setup_inputs(seed, part) draws one part's arguments, and reference() takes and returns one part's arrays. A program takes and returns all parts, laid end to end along the dimension named above; an argument that names none is the same for every part.
All inputs are finite; a program needn't handle non-finite values.
Results may differ from the reference program's by a relative error of at most 0.02.
Values are sent between devices in bfloat16 or wider.
A program may use at most 768 MiB of HBM per device.

```python
import jax
import jax.numpy as jnp
from jax import lax

D = 3840
HEADS = 16
KV_HEADS = 8
HEAD = 256
FF = 15360
WINDOW = 1024
BATCH = 2
CTX = 4096

SOFT_CAP = 50.0
NORM_EPS = 1e-6
ROPE_BASE = 10000.0
NEG_FILL = -1e30


def draw_positions(pos_key):
    draw_key, row_key = jax.random.split(pos_key)
    drawn_pos = jax.random.randint(draw_key, (BATCH,), WINDOW, CTX, dtype=jnp.int32)
    top_row = jax.random.randint(row_key, (), 0, BATCH, dtype=jnp.int32)
    row_ids = jnp.arange(BATCH, dtype=jnp.int32)
    return jnp.where(row_ids == top_row, CTX - 1, drawn_pos).astype(jnp.int32)


def normal_bf16(rand_key, arr_shape, std_scale):
    return (jax.random.normal(rand_key, arr_shape, jnp.float32) * std_scale).astype(jnp.bfloat16)


def setup_inputs(seed: int = 0, part: int = 0) -> dict:
    part_key = jax.random.fold_in(jax.random.key(seed), part)
    row_keys = jax.random.split(part_key, 6)
    weight_keys = jax.random.split(jax.random.key(seed + 1), 8)
    value_gain = jnp.sqrt(jnp.array([WINDOW, CTX], dtype=jnp.float32)).reshape(2, 1, 1)
    return {
        'hidden': normal_bf16(row_keys[0], (BATCH, D), 1.0),
        'positions': draw_positions(row_keys[1]),
        'k_local': normal_bf16(row_keys[2], (BATCH, WINDOW, KV_HEADS, HEAD), 1.0),
        'v_local': normal_bf16(row_keys[3], (BATCH, WINDOW, KV_HEADS, HEAD), 1.0),
        'k_global': normal_bf16(row_keys[4], (BATCH, CTX, KV_HEADS, HEAD), 1.0),
        'v_global': normal_bf16(row_keys[5], (BATCH, CTX, KV_HEADS, HEAD), 1.0),
        'w_query': normal_bf16(weight_keys[0], (2, D, HEADS * HEAD), D ** -0.5),
        'w_key': normal_bf16(weight_keys[1], (2, D, KV_HEADS * HEAD), D ** -0.5),
        'w_value': normal_bf16(weight_keys[2], (2, D, KV_HEADS * HEAD), value_gain * D ** -0.5),
        'w_out': normal_bf16(weight_keys[3], (2, HEADS * HEAD, D), (HEADS * HEAD) ** -0.5),
        'w_gate': normal_bf16(weight_keys[4], (2, D, FF), D ** -0.5),
        'w_up': normal_bf16(weight_keys[5], (2, D, FF), D ** -0.5),
        'w_down': normal_bf16(weight_keys[6], (2, FF, D), FF ** -0.5),
        'norm_scale': jax.random.normal(weight_keys[7], (2, 4, D), jnp.float32) * 0.4,
    }


def rms_norm(values, gain_row):
    values_f32 = values.astype(jnp.float32)
    inv_rms = lax.rsqrt(jnp.mean(values_f32 * values_f32, axis=-1, keepdims=True) + NORM_EPS)
    return (values_f32 * inv_rms * (1.0 + gain_row)).astype(jnp.bfloat16)


def rotary(projected, positions):
    half_dim = HEAD // 2
    inv_freq = ROPE_BASE ** (-2.0 * jnp.arange(half_dim, dtype=jnp.float32) / HEAD)
    angles = positions.astype(jnp.float32)[:, None, None] * inv_freq
    cos_part = jnp.cos(angles)
    sin_part = jnp.sin(angles)
    first_half = projected[..., :half_dim]
    second_half = projected[..., half_dim:]
    return jnp.concatenate([first_half * cos_part - second_half * sin_part, second_half * cos_part + first_half * sin_part], axis=-1)


def attend_row(row_args):
    queries, key_rows, value_rows, key_valid = row_args
    logits = jnp.einsum('grd,ngd->grn', queries.astype(jnp.float32), key_rows.astype(jnp.float32)) * HEAD ** -0.5
    logits = SOFT_CAP * jnp.tanh(logits / SOFT_CAP)
    logits = jnp.where(key_valid[None, None, :], logits, NEG_FILL)
    attn_probs = jax.nn.softmax(logits, axis=-1).astype(jnp.bfloat16)
    mixed_heads = jnp.einsum('grn,ngd->grd', attn_probs.astype(jnp.float32), value_rows.astype(jnp.float32))
    return mixed_heads.astype(jnp.bfloat16)


def add_normed(hidden, branch_sum, gain_row):
    return (hidden.astype(jnp.float32) + rms_norm(branch_sum, gain_row).astype(jnp.float32)).astype(jnp.bfloat16)


def decoder_layer(hidden, positions, k_cache, v_cache, slot_ids, key_valid, layer_weights, gains):
    w_query, w_key, w_value, w_out, w_gate, w_up, w_down = layer_weights
    normed = rms_norm(hidden, gains[0])
    queries = jnp.dot(normed, w_query, preferred_element_type=jnp.float32).reshape(BATCH, HEADS, HEAD)
    key_new = jnp.dot(normed, w_key, preferred_element_type=jnp.float32).reshape(BATCH, KV_HEADS, HEAD)
    value_new = jnp.dot(normed, w_value, preferred_element_type=jnp.float32).astype(jnp.bfloat16).reshape(BATCH, KV_HEADS, HEAD)
    queries = rotary(queries, positions).astype(jnp.bfloat16)
    key_new = rotary(key_new, positions).astype(jnp.bfloat16)
    slot_hit = (jnp.arange(k_cache.shape[1])[None, :] == slot_ids[:, None])[:, :, None, None]
    k_cache = jnp.where(slot_hit, key_new[:, None], k_cache)
    v_cache = jnp.where(slot_hit, value_new[:, None], v_cache)
    grouped = queries.reshape(BATCH, KV_HEADS, HEADS // KV_HEADS, HEAD)
    mixed_heads = lax.map(attend_row, (grouped, k_cache, v_cache, key_valid))
    attn_sum = jnp.dot(mixed_heads.reshape(BATCH, HEADS * HEAD), w_out, preferred_element_type=jnp.float32)
    hidden = add_normed(hidden, attn_sum, gains[1])
    normed = rms_norm(hidden, gains[2])
    gate_proj = jnp.dot(normed, w_gate, preferred_element_type=jnp.float32)
    up_proj = jnp.dot(normed, w_up, preferred_element_type=jnp.float32)
    hidden_act = (jax.nn.gelu(gate_proj, approximate=True) * up_proj).astype(jnp.bfloat16)
    down_sum = jnp.dot(hidden_act, w_down, preferred_element_type=jnp.float32)
    hidden = add_normed(hidden, down_sum, gains[3])
    return hidden, k_cache, v_cache


def reference(hidden, positions, k_local, v_local, k_global, v_global, w_query, w_key, w_value, w_out, w_gate, w_up, w_down, norm_scale):
    stacks = (w_query, w_key, w_value, w_out, w_gate, w_up, w_down)
    local_valid = jnp.full((BATCH, WINDOW), True)
    global_valid = jnp.arange(CTX)[None, :] <= positions[:, None]
    hidden, k_local, v_local = decoder_layer(hidden, positions, k_local, v_local, positions % WINDOW, local_valid, tuple(stacked[0] for stacked in stacks), norm_scale[0])
    hidden, k_global, v_global = decoder_layer(hidden, positions, k_global, v_global, positions, global_valid, tuple(stacked[1] for stacked in stacks), norm_scale[1])
    return (hidden, k_local, v_local, k_global, v_global)
```

```python
import functools

import jax
import jax.numpy as jnp
from jax import lax
from jax.experimental import pallas as pl
from jax.experimental.pallas import tpu as pltpu
from jax.sharding import PartitionSpec as P

SOFT_CAP = 50.0
NORM_EPS = 1e-6
ROPE_BASE = 10000.0

CHUNK = 256
SLOTS = 18
QKV_PARTS = 5
KV_STEP = 1024

F32 = jnp.float32
BF16 = jnp.bfloat16
MESH = pl.DeviceIdType.MESH


def rms_norm(values, gain_row):
    inv_rms = lax.rsqrt(jnp.mean(values * values, axis=-1, keepdims=True) + NORM_EPS)
    return (values * inv_rms * (1.0 + gain_row)).astype(BF16)


def step_kernel(n_tp, pos_ref, hid_ref, cos_ref, sin_ref, norm_ref, kl_in, vl_in, kg_in, vg_in, wq, wk, wv, wo, wg, wu, wd,
                hid_out, kl, vl, kg, vg,
                ring, bq, bk, bv, x_ref, a_ref, o_ref, h_ref, acc, e_ref, part,
                ring_sem, qkv_sem, cache_sem, send_sem, recv_sem):
    rows, width = hid_ref.shape
    head = kl.shape[2]
    half = head // 2
    ff = wg.shape[2]
    layers = wg.shape[0]
    n_wo = wo.shape[1] // CHUNK
    n_gu = width // CHUNK
    n_dn = ff // CHUNK
    dn_rest = ff - n_dn * CHUNK
    at_gu, at_dn = n_wo, n_wo + n_gu
    per_layer = n_wo + n_gu + n_dn + (1 if dn_rest else 0)
    n_chunks = layers * per_layer
    me = lax.axis_index('tp')

    def chunk_copies(kind, layer, k, slot):
        if kind == 'wo':
            return [pltpu.make_async_copy(wo.at[layer, pl.ds(k * CHUNK, CHUNK)], ring.at[slot], ring_sem.at[slot, 0])]
        if kind == 'gu':
            return [
                pltpu.make_async_copy(wg.at[layer, pl.ds(k * CHUNK, CHUNK)], ring.at[slot, :, pl.ds(0, ff)], ring_sem.at[slot, 0]),
                pltpu.make_async_copy(wu.at[layer, pl.ds(k * CHUNK, CHUNK)], ring.at[slot, :, pl.ds(ff, ff)], ring_sem.at[slot, 1]),
            ]
        if kind == 'dn':
            return [pltpu.make_async_copy(wd.at[layer, pl.ds(k * CHUNK, CHUNK)], ring.at[slot], ring_sem.at[slot, 0])]
        return [pltpu.make_async_copy(wd.at[layer, pl.ds(n_dn * CHUNK, dn_rest)], ring.at[slot, pl.ds(0, dn_rest)], ring_sem.at[slot, 0])]

    def start_chunk(c):
        slot = lax.rem(c, SLOTS)
        layer = c // per_layer
        r = c - layer * per_layer

        def go(kind, k):
            for copy in chunk_copies(kind, layer, k, slot):
                copy.start()

        if isinstance(c, int):
            if r < at_gu:
                go('wo', r)
            elif r < at_dn:
                go('gu', r - at_gu)
            elif r < at_dn + n_dn:
                go('dn', r - at_dn)
            else:
                go('rest', 0)
            return
        live = c < n_chunks
        pl.when(live & (r < at_gu))(lambda: go('wo', r))
        pl.when(live & (r >= at_gu) & (r < at_dn))(lambda: go('gu', r - at_gu))
        pl.when(live & (r >= at_dn) & (r < at_dn + n_dn))(lambda: go('dn', r - at_dn))
        if dn_rest:
            pl.when(live & (r == at_dn + n_dn))(lambda: go('rest', 0))

    def stream_dot(kind, layer, lhs_ref, first, count):
        def body(k, carry):
            c = layer * per_layer + first + k
            slot = lax.rem(c, SLOTS)
            for copy in chunk_copies(kind, layer, k, slot):
                copy.wait()
            lhs = lhs_ref[:, pl.ds(pl.multiple_of(k * CHUNK, CHUNK), CHUNK)]
            acc[...] += jnp.dot(lhs, ring[slot], preferred_element_type=F32)
            start_chunk(c + SLOTS)
            return carry

        lax.fori_loop(0, count, body, 0)

    qkv_rows = width // QKV_PARTS

    def qkv_copies(layer, j):
        piece = pl.ds(j * qkv_rows, qkv_rows)
        return [pltpu.make_async_copy(src.at[layer, piece], dst.at[piece], qkv_sem.at[i, j])
                for i, (src, dst) in enumerate(((wq, bq), (wk, bk), (wv, bv)))]

    def cache_copies(layer):
        pairs = ((kl_in, kl), (vl_in, vl)) if layer == 0 else ((kg_in, kg), (vg_in, vg))
        return [pltpu.make_async_copy(src.at[b], dst.at[b], cache_sem.at[layer, i, b])
                for i, (src, dst) in enumerate(pairs) for b in range(rows)]

    def send_copies(phase):
        copies = []
        for step in range(1, n_tp):
            peer = lax.rem(me + step, n_tp)
            copies.append(pltpu.make_async_remote_copy(
                src_ref=part.at[phase, me], dst_ref=part.at[phase, me],
                send_sem=send_sem.at[phase, step - 1], recv_sem=recv_sem.at[phase, step - 1],
                device_id={'tp': peer}, device_id_type=MESH))
        return copies

    def exchange(phase):
        part[phase, me] = acc[...].astype(BF16)
        copies = send_copies(phase)
        for copy in copies:
            copy.start()
        for copy in copies:
            copy.wait_recv()
        total = part[phase, 0].astype(F32)
        for j in range(1, n_tp):
            total = total + part[phase, j].astype(F32)
        return total

    def gain(layer, i):
        return norm_ref[layer, pl.ds(i, 1), :]

    def add_normed(layer, i, branch_sum):
        x = (x_ref[...] + rms_norm(branch_sum, gain(layer, i)).astype(F32)).astype(BF16)
        x_ref[...] = x.astype(F32)
        return x

    def rotate(values):
        first, second = values[:, :half], values[:, half:]
        cos_part, sin_part = cos_ref[...], sin_ref[...]
        return jnp.concatenate([first * cos_part - second * sin_part, second * cos_part + first * sin_part], axis=-1)

    def store_row(cache, b, slot, new_row):
        n = cache.shape[1]
        step = min(n, KV_STEP)

        def body(i, carry):
            piece = pl.ds(pl.multiple_of(i * step, step), step)
            ids = lax.broadcasted_iota(jnp.int32, (step, head), 0) + i * step
            cache[b, piece] = jnp.where(ids == slot, jnp.broadcast_to(new_row, (step, head)), cache[b, piece])
            return carry

        lax.fori_loop(0, n // step, body, 0)

    def attention(layer, kc, vc):
        n = kc.shape[1]
        a_ref[...] = rms_norm(x_ref[...], gain(layer, 0))
        hq = bq.shape[1]

        def qkv_body(j, carry):
            q, k, v = carry
            for copy in qkv_copies(layer, j):
                copy.wait()
            piece = pl.ds(pl.multiple_of(j * qkv_rows, qkv_rows), qkv_rows)
            lhs = a_ref[:, piece]
            q = q + jnp.dot(lhs, bq[piece], preferred_element_type=F32)
            k = k + jnp.dot(lhs, bk[piece], preferred_element_type=F32)
            v = v + jnp.dot(lhs, bv[piece], preferred_element_type=F32)
            return q, k, v

        q, k, v = lax.fori_loop(0, QKV_PARTS, qkv_body, (
            jnp.zeros((rows, hq), F32), jnp.zeros((rows, head), F32), jnp.zeros((rows, head), F32)))
        if layer + 1 < layers:
            for j in range(QKV_PARTS):
                for copy in qkv_copies(layer + 1, j):
                    copy.start()
        group = hq // head
        queries = jnp.concatenate([rotate(q[:, g * head:(g + 1) * head]) for g in range(group)], axis=0).astype(BF16)
        k_new = rotate(k).astype(BF16)
        v_new = v.astype(BF16)
        for copy in cache_copies(layer):
            copy.wait()
        for b in range(rows):
            slot = lax.rem(pos_ref[b], n)
            store_row(kc, b, slot, k_new[b:b + 1])
            store_row(vc, b, slot, v_new[b:b + 1])
        q_rows = group * rows
        row_seq = lax.rem(lax.broadcasted_iota(jnp.int32, (q_rows, 1), 0), rows)
        last = jnp.zeros((q_rows, 1), jnp.int32)
        for b in range(rows):
            last = jnp.where(row_seq == b, pos_ref[b], last)

        def pick(per_seq):
            out = per_seq[0]
            for b in range(1, rows):
                out = jnp.where(row_seq == b, per_seq[b], out)
            return out

        step = min(n, KV_STEP)
        contract_last = (((1,), (1,)), ((), ()))

        def score_body(i, total):
            piece = pl.ds(pl.multiple_of(i * step, step), step)
            s = pick([lax.dot_general(queries, kc[b, piece], contract_last, preferred_element_type=F32) for b in range(rows)])
            s = s * head ** -0.5
            e = jnp.exp(SOFT_CAP * jnp.tanh(s / SOFT_CAP))
            ids = lax.broadcasted_iota(jnp.int32, (q_rows, step), 1) + i * step
            e = jnp.where(ids <= last, e, 0.0)
            e_ref[:, piece] = e
            return total + jnp.sum(e, axis=-1, keepdims=True)

        total = lax.fori_loop(0, n // step, score_body, jnp.zeros((q_rows, 1), F32))

        def value_body(i, out):
            piece = pl.ds(pl.multiple_of(i * step, step), step)
            probs = (e_ref[:, piece] / total).astype(BF16)
            return out + pick([jnp.dot(probs, vc[b, piece], preferred_element_type=F32) for b in range(rows)])

        mixed = lax.fori_loop(0, n // step, value_body, jnp.zeros((q_rows, head), F32)).astype(BF16)
        for g in range(group):
            o_ref[:, pl.ds(g * head, head)] = mixed[g * rows:(g + 1) * rows]

    for j in range(QKV_PARTS):
        for copy in qkv_copies(0, j):
            copy.start()
    for copy in cache_copies(0):
        copy.start()
    for c in range(min(SLOTS, n_chunks)):
        start_chunk(c)
    for copy in cache_copies(1):
        copy.start()

    barrier = pltpu.get_barrier_semaphore()
    for step in range(1, n_tp):
        pl.semaphore_signal(barrier, inc=1, device_id={'tp': lax.rem(me + step, n_tp)}, device_id_type=MESH)

    x_ref[...] = hid_ref[...].astype(F32)
    for layer in range(layers):
        kc, vc = (kl, vl) if layer == 0 else (kg, vg)
        attention(layer, kc, vc)
        acc[...] = jnp.zeros_like(acc)
        stream_dot('wo', layer, o_ref, 0, n_wo)
        if layer == 0:
            pl.semaphore_wait(barrier, n_tp - 1)
        x = add_normed(layer, 1, exchange(2 * layer))
        a_ref[...] = rms_norm(x.astype(F32), gain(layer, 2))
        acc[...] = jnp.zeros_like(acc)
        stream_dot('gu', layer, a_ref, at_gu, n_gu)
        gate_up = acc[...]
        h_ref[...] = (jax.nn.gelu(gate_up[:, :ff], approximate=True) * gate_up[:, ff:]).astype(BF16)
        acc[...] = jnp.zeros_like(acc)
        stream_dot('dn', layer, h_ref, at_dn, n_dn)
        if dn_rest:
            c = layer * per_layer + per_layer - 1
            slot = c % SLOTS
            for copy in chunk_copies('rest', layer, 0, slot):
                copy.wait()
            acc[...] += jnp.dot(h_ref[:, pl.ds(n_dn * CHUNK, dn_rest)], ring[slot, pl.ds(0, dn_rest)], preferred_element_type=F32)
            if c + SLOTS < n_chunks:
                start_chunk(c + SLOTS)
        x = add_normed(layer, 3, exchange(2 * layer + 1))
    hid_out[...] = x
    for phase in range(2 * layers):
        for copy in send_copies(phase):
            copy.wait_send()


def decode_step(n_tp, hidden, positions, k_local, v_local, k_global, v_global, w_query, w_key, w_value, w_out, w_gate, w_up, w_down, norm_scale):
    rows, width = hidden.shape
    caches = [c.reshape(c.shape[0], c.shape[1], c.shape[3]) for c in (k_local, v_local, k_global, v_global)]
    head = caches[0].shape[2]
    half = head // 2
    inv_freq = ROPE_BASE ** (-2.0 * jnp.arange(half, dtype=F32) / head)
    angles = positions.astype(F32)[:, None] * inv_freq
    cos_part, sin_part = jnp.cos(angles), jnp.sin(angles)
    hq, ff, layers = w_query.shape[2], w_gate.shape[2], w_gate.shape[0]
    n_ctx = max(c.shape[1] for c in caches)
    vmem = pl.BlockSpec(memory_space=pltpu.VMEM)
    hbm = pl.BlockSpec(memory_space=pl.ANY)
    smem = pl.BlockSpec(memory_space=pltpu.SMEM)
    outs = pl.pallas_call(
        functools.partial(step_kernel, n_tp),
        out_shape=(jax.ShapeDtypeStruct(hidden.shape, BF16),) + tuple(jax.ShapeDtypeStruct(c.shape, BF16) for c in caches),
        in_specs=[smem] + [vmem] * 4 + [hbm] * 11,
        out_specs=(vmem,) * 5,
        scratch_shapes=[
            pltpu.VMEM((SLOTS, CHUNK, width), BF16),
            pltpu.VMEM((width, hq), BF16),
            pltpu.VMEM((width, head), BF16),
            pltpu.VMEM((width, head), BF16),
            pltpu.VMEM((rows, width), F32),
            pltpu.VMEM((rows, width), BF16),
            pltpu.VMEM((rows, hq), BF16),
            pltpu.VMEM((rows, ff), BF16),
            pltpu.VMEM((rows, 2 * ff), F32),
            pltpu.VMEM((hq // head * rows, n_ctx), F32),
            pltpu.VMEM((2 * layers, n_tp, rows, width), BF16),
            pltpu.SemaphoreType.DMA((SLOTS, 2)),
            pltpu.SemaphoreType.DMA((3, QKV_PARTS)),
            pltpu.SemaphoreType.DMA((2, 2, rows)),
            pltpu.SemaphoreType.DMA((2 * layers, n_tp - 1)),
            pltpu.SemaphoreType.DMA((2 * layers, n_tp - 1)),
        ],
        compiler_params=pltpu.CompilerParams(
            collective_id=0, has_side_effects=True, vmem_limit_bytes=56 * 1024 * 1024),
        name='decode_step',
    )(positions, hidden, cos_part, sin_part, norm_scale, *caches, w_query, w_key, w_value, w_out, w_gate, w_up, w_down)
    hidden_out = outs[0]
    new_caches = [c.reshape(old.shape) for c, old in zip(outs[1:], (k_local, v_local, k_global, v_global))]
    return (hidden_out, *new_caches)


def solution(mesh):
    row_spec = P('dp', None)
    cache_spec = P('dp', None, 'tp', None)
    col_split = P(None, None, 'tp')
    row_split = P(None, 'tp', None)
    in_specs = (row_spec, P('dp'), cache_spec, cache_spec, cache_spec, cache_spec, col_split, col_split, col_split, row_split, col_split, col_split, row_split, P())
    out_specs = (row_spec, cache_spec, cache_spec, cache_spec, cache_spec)
    return jax.shard_map(functools.partial(decode_step, mesh.shape['tp']), mesh=mesh, in_specs=in_specs, out_specs=out_specs, check_vma=False)
```

```python
import functools

import jax
import jax.numpy as jnp
import numpy as np
from jax import lax
from jax.experimental import pallas as pl
from jax.experimental.pallas import tpu as pltpu
from jax.sharding import PartitionSpec as P

SOFT_CAP = 50.0
NORM_EPS = 1e-6
ROPE_BASE = 10000.0

CHUNK = 256
SLOTS = 22
QKV_PARTS = 5
KV_STEP = 1024
GU_GROUP = 5
DN_GROUP = 3

VMEM_LIMIT = 52 * 1024 * 1024

F32 = jnp.float32
BF16 = jnp.bfloat16
MESH = pl.DeviceIdType.MESH


def rem(a, b):
    return a % b if isinstance(a, int) else lax.rem(a, b)


def rms_norm(values, gain_row):
    inv_rms = lax.rsqrt(jnp.mean(values * values, axis=-1, keepdims=True) + NORM_EPS)
    return (values * inv_rms * (1.0 + gain_row)).astype(BF16)


def step_kernel(n_tp, pos_in, hid_in, freq_in, norm_in, kl_in, vl_in, kg_in, vg_in, wq, wk, wv, wo, wg, wu, wd,
                hid_out, kl, vl, kg, vg,
                pos_ref, hid_ref, freq_ref, norm_ref, ring, bq, bk, bv, x_ref, a_ref, o_ref, h_ref, acc, e_ref, part,
                small_sem, ring_sem, qkv_sem, cache_sem, send_sem, recv_sem):
    rows, width = hid_ref.shape
    head = kl.shape[2]
    half = head // 2
    ff = wg.shape[2]
    layers = wg.shape[0]
    n_wo = wo.shape[1] // CHUNK
    n_gu = width // CHUNK
    n_dn = ff // CHUNK
    dn_rest = ff - n_dn * CHUNK
    at_gu, at_dn = n_wo, n_wo + n_gu
    per_layer = n_wo + n_gu + n_dn + (1 if dn_rest else 0)
    n_chunks = layers * per_layer
    me = lax.axis_index('tp')

    def chunk_copies(kind, layer, k, slot):
        if kind == 'wo':
            return [pltpu.make_async_copy(wo.at[layer, pl.ds(k * CHUNK, CHUNK)], ring.at[slot], ring_sem.at[slot, 0])]
        if kind == 'gu':
            return [
                pltpu.make_async_copy(wg.at[layer, pl.ds(k * CHUNK, CHUNK)], ring.at[slot, :, pl.ds(0, ff)], ring_sem.at[slot, 0]),
                pltpu.make_async_copy(wu.at[layer, pl.ds(k * CHUNK, CHUNK)], ring.at[slot, :, pl.ds(ff, ff)], ring_sem.at[slot, 1]),
            ]
        if kind == 'dn':
            return [pltpu.make_async_copy(wd.at[layer, pl.ds(k * CHUNK, CHUNK)], ring.at[slot], ring_sem.at[slot, 0])]
        return [pltpu.make_async_copy(wd.at[layer, pl.ds(n_dn * CHUNK, dn_rest)], ring.at[slot, pl.ds(0, dn_rest)], ring_sem.at[slot, 0])]

    def start_chunk(c):
        slot = rem(c, SLOTS)
        layer = c // per_layer
        r = c - layer * per_layer

        def go(kind, k):
            for copy in chunk_copies(kind, layer, k, slot):
                copy.start()

        if isinstance(c, int):
            if c >= n_chunks:
                return
            if r < at_gu:
                go('wo', r)
            elif r < at_dn:
                go('gu', r - at_gu)
            elif r < at_dn + n_dn:
                go('dn', r - at_dn)
            else:
                go('rest', 0)
            return
        live = c < n_chunks
        pl.when(live & (r < at_gu))(lambda: go('wo', r))
        pl.when(live & (r >= at_gu) & (r < at_dn))(lambda: go('gu', r - at_gu))
        pl.when(live & (r >= at_dn) & (r < at_dn + n_dn))(lambda: go('dn', r - at_dn))
        if dn_rest:
            pl.when(live & (r == at_dn + n_dn))(lambda: go('rest', 0))

    def group_dot(kind, layer, lhs_ref, first, k0, group, rest=False):
        base = layer * per_layer + first + k0
        slots = [rem(base + j, SLOTS) for j in range(group)]
        for j, slot in enumerate(slots):
            for copy in chunk_copies(kind, layer, k0 + j, slot):
                copy.wait()
        out = acc[...]
        if rest:
            rest_slot = rem(base + group, SLOTS)
            for copy in chunk_copies('rest', layer, 0, rest_slot):
                copy.wait()
        for j, slot in enumerate(slots):
            at = (k0 + j) * CHUNK
            lhs = lhs_ref[:, pl.ds(at if isinstance(at, int) else pl.multiple_of(at, CHUNK), CHUNK)]
            out = out + jnp.dot(lhs, ring[slot], preferred_element_type=F32)
        if rest:
            out = out + jnp.dot(lhs_ref[:, pl.ds(n_dn * CHUNK, dn_rest)], ring[rest_slot, pl.ds(0, dn_rest)], preferred_element_type=F32)
        acc[...] = out
        for j in range(group + (1 if rest else 0)):
            start_chunk(base + j + SLOTS)

    def stream_dot(kind, layer, lhs_ref, first, count, group, rest=False):
        acc[...] = jnp.zeros_like(acc)
        steps, left = divmod(count, group)
        if rest and not left:
            steps, left = steps - 1, group

        def body(i, carry):
            group_dot(kind, layer, lhs_ref, first, i * group, group)
            return carry

        if steps == 1:
            body(0, 0)
        else:
            lax.fori_loop(0, steps, body, 0)
        if left or rest:
            group_dot(kind, layer, lhs_ref, first, steps * group, left, rest)

    qkv_rows = width // QKV_PARTS

    def qkv_copies(layer, j):
        piece = pl.ds(j * qkv_rows, qkv_rows)
        return [pltpu.make_async_copy(src.at[layer, piece], dst.at[piece], qkv_sem.at[i, j])
                for i, (src, dst) in enumerate(((wq, bq), (wk, bk), (wv, bv)))]

    def cache_copies(layer):
        pairs = ((kl_in, kl), (vl_in, vl)) if layer == 0 else ((kg_in, kg), (vg_in, vg))
        return [pltpu.make_async_copy(src.at[b], dst.at[b], cache_sem.at[layer, i, b])
                for i, (src, dst) in enumerate(pairs) for b in range(rows)]

    def send_copies(phase):
        copies = []
        for step in range(1, n_tp):
            peer = lax.rem(me + step, n_tp)
            copies.append(pltpu.make_async_remote_copy(
                src_ref=part.at[phase, me], dst_ref=part.at[phase, me],
                send_sem=send_sem.at[phase, step - 1], recv_sem=recv_sem.at[phase, step - 1],
                device_id={'tp': peer}, device_id_type=MESH))
        return copies

    def exchange(phase, meanwhile=None):
        part[phase, me] = acc[...].astype(BF16)
        copies = send_copies(phase)
        for copy in copies:
            copy.start()
        if meanwhile is not None:
            meanwhile()
        for copy in copies:
            copy.wait_recv()
        total = part[phase, 0].astype(F32)
        for j in range(1, n_tp):
            total = total + part[phase, j].astype(F32)
        return total

    def gain(layer, i):
        return norm_ref[layer, pl.ds(i, 1), :]

    def add_normed(layer, i, branch_sum):
        x = (x_ref[...] + rms_norm(branch_sum, gain(layer, i)).astype(F32)).astype(BF16)
        x_ref[...] = x.astype(F32)
        return x

    def rotate(values, trig):
        first, second = values[:, :half], values[:, half:]
        cos_part, sin_part = trig
        return jnp.concatenate([first * cos_part - second * sin_part, second * cos_part + first * sin_part], axis=-1)

    def store_row(cache, b, slot, new_row):
        n = cache.shape[1]
        step = min(n, KV_STEP)

        def body(i, carry):
            piece = pl.ds(pl.multiple_of(i * step, step), step)
            ids = lax.broadcasted_iota(jnp.int32, (step, head), 0) + i * step
            cache[b, piece] = jnp.where(ids == slot, jnp.broadcast_to(new_row, (step, head)), cache[b, piece])
            return carry

        lax.fori_loop(0, n // step, body, 0)

    def attention(layer, kc, vc, trig):
        n = kc.shape[1]
        a_ref[...] = rms_norm(x_ref[...], gain(layer, 0))
        hq = bq.shape[1]

        q, k, v = jnp.zeros((rows, hq), F32), jnp.zeros((rows, head), F32), jnp.zeros((rows, head), F32)
        if layer > 0:
            for j in range(QKV_PARTS):
                for copy in qkv_copies(layer, j):
                    copy.wait()
        for j in range(QKV_PARTS):
            if layer == 0:
                for copy in qkv_copies(layer, j):
                    copy.wait()
            piece = pl.ds(j * qkv_rows, qkv_rows)
            lhs = a_ref[:, piece]
            q = q + jnp.dot(lhs, bq[piece], preferred_element_type=F32)
            k = k + jnp.dot(lhs, bk[piece], preferred_element_type=F32)
            v = v + jnp.dot(lhs, bv[piece], preferred_element_type=F32)
        if layer + 1 < layers:
            for j in range(QKV_PARTS):
                for copy in qkv_copies(layer + 1, j):
                    copy.start()
        group = hq // head
        queries = jnp.concatenate([rotate(q[:, g * head:(g + 1) * head], trig) for g in range(group)], axis=0).astype(BF16)
        k_new = rotate(k, trig).astype(BF16)
        v_new = v.astype(BF16)
        for copy in cache_copies(layer):
            copy.wait()
        q_rows = group * rows
        row_seq = lax.rem(lax.broadcasted_iota(jnp.int32, (q_rows, 1), 0), rows)
        last, slot = jnp.zeros((q_rows, 1), jnp.int32), jnp.zeros((q_rows, 1), jnp.int32)
        for b in range(rows):
            last = jnp.where(row_seq == b, pos_ref[b], last)
            slot = jnp.where(row_seq == b, lax.rem(pos_ref[b], n), slot)

        def pick(per_seq):
            out = per_seq[0]
            for b in range(1, rows):
                out = jnp.where(row_seq == b, per_seq[b], out)
            return out

        step = min(n, KV_STEP)
        contract_last = (((1,), (1,)), ((), ()))

        def soft_exp(s):
            return jnp.exp(SOFT_CAP * jnp.tanh(s * head ** -0.5 / SOFT_CAP))

        per_row = [jnp.concatenate([new.astype(F32)] * group, axis=0) for new in (k_new, v_new)]
        e_new = soft_exp(jnp.sum(queries.astype(F32) * per_row[0], axis=-1, keepdims=True))
        total = e_new
        weights = []
        for i in range(n // step):
            piece = pl.ds(i * step, step)
            s = pick([lax.dot_general(queries, kc[b, piece], contract_last, preferred_element_type=F32) for b in range(rows)])
            ids = lax.broadcasted_iota(jnp.int32, (q_rows, step), 1) + i * step
            e = jnp.where((ids <= last) & (ids != slot), soft_exp(s), 0.0)
            e_ref[:, piece] = e
            total = total + jnp.sum(e, axis=-1, keepdims=True)
        out = (e_new / total).astype(BF16).astype(F32) * per_row[1]
        for i in range(n // step):
            piece = pl.ds(i * step, step)
            probs = (e_ref[:, piece] / total).astype(BF16)
            out = out + pick([jnp.dot(probs, vc[b, piece], preferred_element_type=F32) for b in range(rows)])
        mixed = out.astype(BF16)
        for g in range(group):
            o_ref[:, pl.ds(g * head, head)] = mixed[g * rows:(g + 1) * rows]

        def store_new():
            for b in range(rows):
                store_row(kc, b, lax.rem(pos_ref[b], n), k_new[b:b + 1])
                store_row(vc, b, lax.rem(pos_ref[b], n), v_new[b:b + 1])

        return store_new

    small = [pltpu.make_async_copy(src, dst, small_sem.at[i]) for i, (src, dst) in enumerate(
        ((hid_in, hid_ref), (norm_in, norm_ref), (pos_in, pos_ref), (freq_in, freq_ref)))]
    for copy in small:
        copy.start()
    for j in range(QKV_PARTS):
        for copy in qkv_copies(0, j):
            copy.start()
    for copy in cache_copies(0):
        copy.start()
    for c in range(min(SLOTS, n_chunks)):
        start_chunk(c)
    for copy in cache_copies(1):
        copy.start()

    barrier = pltpu.get_barrier_semaphore()
    for step in range(1, n_tp):
        pl.semaphore_signal(barrier, inc=1, device_id={'tp': lax.rem(me + step, n_tp)}, device_id_type=MESH)

    for copy in small:
        copy.wait()
    x_ref[...] = hid_ref[...].astype(F32)
    row_ids = lax.broadcasted_iota(jnp.int32, (rows, half), 0)
    pos_rows = jnp.zeros((rows, half), F32)
    for b in range(rows):
        pos_rows = jnp.where(row_ids == b, pos_ref[b].astype(F32), pos_rows)
    angles = pos_rows * freq_ref[...]
    trig = jnp.cos(angles), jnp.sin(angles)
    for layer in range(layers):
        kc, vc = (kl, vl) if layer == 0 else (kg, vg)
        store_new = attention(layer, kc, vc, trig)
        stream_dot('wo', layer, o_ref, 0, n_wo, n_wo)
        if layer == 0:
            pl.semaphore_wait(barrier, n_tp - 1)
        x = add_normed(layer, 1, exchange(2 * layer, store_new))
        a_ref[...] = rms_norm(x.astype(F32), gain(layer, 2))
        stream_dot('gu', layer, a_ref, at_gu, n_gu, GU_GROUP)
        gate_up = acc[...]
        h_ref[...] = (jax.nn.gelu(gate_up[:, :ff], approximate=True) * gate_up[:, ff:]).astype(BF16)
        stream_dot('dn', layer, h_ref, at_dn, n_dn, DN_GROUP, dn_rest > 0)
        x = add_normed(layer, 3, exchange(2 * layer + 1))
    hid_out[...] = x
    for phase in range(2 * layers):
        for copy in send_copies(phase):
            copy.wait_send()


def write_kernel(*refs):
    n = len(refs) // 2
    copies = [pltpu.make_async_copy(refs[i], refs[n + i], refs[-1].at[i]) for i in range(n)]
    for copy in copies:
        copy.start()
    for copy in copies:
        copy.wait()


def decode_step(n_tp, hidden, positions, k_local, v_local, k_global, v_global, w_query, w_key, w_value, w_out, w_gate, w_up, w_down, norm_scale):
    rows, width = hidden.shape
    caches = [c.reshape(c.shape[0], c.shape[1], c.shape[3]) for c in (k_local, v_local, k_global, v_global)]
    head = caches[0].shape[2]
    half = head // 2
    inv_freq = jnp.asarray(ROPE_BASE ** (-2.0 * np.arange(half) / head), F32)[None, :]
    hq, ff, layers = w_query.shape[2], w_gate.shape[2], w_gate.shape[0]
    n_ctx = max(c.shape[1] for c in caches)
    vmem = pl.BlockSpec(memory_space=pltpu.VMEM)
    hbm = pl.BlockSpec(memory_space=pl.ANY)
    outs = pl.pallas_call(
        functools.partial(step_kernel, n_tp),
        out_shape=tuple(pltpu.VMEM(a.shape, BF16) for a in (hidden, *caches)),
        in_specs=[hbm] * 15,
        out_specs=(vmem,) * 5,
        scratch_shapes=[
            pltpu.SMEM((rows,), jnp.int32),
            pltpu.VMEM((rows, width), BF16),
            pltpu.VMEM((1, half), F32),
            pltpu.VMEM(norm_scale.shape, F32),
            pltpu.VMEM((SLOTS, CHUNK, width), BF16),
            pltpu.VMEM((width, hq), BF16),
            pltpu.VMEM((width, head), BF16),
            pltpu.VMEM((width, head), BF16),
            pltpu.VMEM((rows, width), F32),
            pltpu.VMEM((rows, width), BF16),
            pltpu.VMEM((rows, hq), BF16),
            pltpu.VMEM((rows, ff), BF16),
            pltpu.VMEM((rows, 2 * ff), F32),
            pltpu.VMEM((hq // head * rows, n_ctx), F32),
            pltpu.VMEM((2 * layers, n_tp, rows, width), BF16),
            pltpu.SemaphoreType.DMA((4,)),
            pltpu.SemaphoreType.DMA((SLOTS, 2)),
            pltpu.SemaphoreType.DMA((3, QKV_PARTS)),
            pltpu.SemaphoreType.DMA((2, 2, rows)),
            pltpu.SemaphoreType.DMA((2 * layers, n_tp - 1)),
            pltpu.SemaphoreType.DMA((2 * layers, n_tp - 1)),
        ],
        compiler_params=pltpu.CompilerParams(
            collective_id=0, has_side_effects=True, vmem_limit_bytes=VMEM_LIMIT),
        name='decode_step',
    )(positions, hidden, inv_freq, norm_scale, *caches, w_query, w_key, w_value, w_out, w_gate, w_up, w_down)
    hidden_out, *new_caches = pl.pallas_call(
        write_kernel,
        out_shape=tuple(jax.ShapeDtypeStruct(o.shape, o.dtype) for o in outs),
        in_specs=[hbm] * len(outs),
        out_specs=(hbm,) * len(outs),
        scratch_shapes=[pltpu.SemaphoreType.DMA((len(outs),))],
        compiler_params=pltpu.CompilerParams(vmem_limit_bytes=1024 * 1024),
        name='write_out',
    )(*outs)
    new_caches = [c.reshape(old.shape) for c, old in zip(new_caches, (k_local, v_local, k_global, v_global))]
    return (hidden_out, *new_caches)


def solution(mesh):
    row_spec = P('dp', None)
    cache_spec = P('dp', None, 'tp', None)
    col_split = P(None, None, 'tp')
    row_split = P(None, 'tp', None)
    in_specs = (row_spec, P('dp'), cache_spec, cache_spec, cache_spec, cache_spec, col_split, col_split, col_split, row_split, col_split, col_split, row_split, P())
    out_specs = (row_spec, cache_spec, cache_spec, cache_spec, cache_spec)
    return jax.shard_map(functools.partial(decode_step, mesh.shape['tp']), mesh=mesh, in_specs=in_specs, out_specs=out_specs, check_vma=False)
```

```python
import functools

import jax
import jax.numpy as jnp
import numpy as np
from jax import lax
from jax.experimental import pallas as pl
from jax.experimental.pallas import tpu as pltpu
from jax.sharding import PartitionSpec as P

SOFT_CAP = 50.0
NORM_EPS = 1e-6
ROPE_BASE = 10000.0

CHUNK = 256
SLOTS = 22
QKV_PARTS = 5
KV_STEP = 1024
GU_GROUP = 5
DN_GROUP = 3
QKV_CHUNKS, CACHE_CHUNKS = 4, 3
START_WINDOW, WINDOW, SUM_WINDOW = 10, 8, 14

VMEM_LIMIT = 52 * 1024 * 1024

F32 = jnp.float32
BF16 = jnp.bfloat16
MESH = pl.DeviceIdType.MESH


def split(count, group):
    return [min(group, count - i) for i in range(0, count, group)]


def rms_norm(values, gain_row):
    inv_rms = lax.rsqrt(jnp.mean(values * values, axis=-1, keepdims=True) + NORM_EPS)
    return (values * inv_rms * (1.0 + gain_row)).astype(BF16)


def step_kernel(n_tp, pos_in, hid_in, freq_in, norm_in, kl_in, vl_in, kg_in, vg_in, wq, wk, wv, wo, wg, wu, wd,
                hid_out, kl, vl, kg, vg,
                pos_ref, hid_ref, freq_ref, norm_ref, ring, bq, bk, bv, x_ref, a_ref, o_ref, h_ref, acc, e_ref, part,
                small_sem, ring_sem, qkv_sem, cache_sem, send_sem, recv_sem):
    rows, width = hid_ref.shape
    head = kl.shape[2]
    half = head // 2
    ff = wg.shape[2]
    layers = wg.shape[0]
    n_wo = wo.shape[1] // CHUNK
    n_gu = width // CHUNK
    n_dn = ff // CHUNK
    dn_rest = ff - n_dn * CHUNK
    at_gu, at_dn = n_wo, n_wo + n_gu
    per_layer = n_wo + n_gu + n_dn + (1 if dn_rest else 0)
    me = lax.axis_index('tp')

    def chunk_copies(kind, layer, k, slot):
        if kind == 'wo':
            return [pltpu.make_async_copy(wo.at[layer, pl.ds(k * CHUNK, CHUNK)], ring.at[slot], ring_sem.at[slot, 0])]
        if kind == 'gu':
            return [
                pltpu.make_async_copy(wg.at[layer, pl.ds(k * CHUNK, CHUNK)], ring.at[slot, :, pl.ds(0, ff)], ring_sem.at[slot, 0]),
                pltpu.make_async_copy(wu.at[layer, pl.ds(k * CHUNK, CHUNK)], ring.at[slot, :, pl.ds(ff, ff)], ring_sem.at[slot, 1]),
            ]
        if kind == 'dn':
            return [pltpu.make_async_copy(wd.at[layer, pl.ds(k * CHUNK, CHUNK)], ring.at[slot], ring_sem.at[slot, 0])]
        return [pltpu.make_async_copy(wd.at[layer, pl.ds(n_dn * CHUNK, dn_rest)], ring.at[slot, pl.ds(0, dn_rest)], ring_sem.at[slot, 0])]

    def chunk_of(c):
        layer, r = divmod(c, per_layer)
        if r < at_gu:
            return 'wo', layer, r
        if r < at_dn:
            return 'gu', layer, r - at_gu
        if r < at_dn + n_dn:
            return 'dn', layer, r - at_dn
        return 'rest', layer, 0

    queue = []
    for layer in range(layers):
        queue += [('qkv', layer), ('cache', layer)]
        queue += [('chunk', c) for c in range(layer * per_layer, (layer + 1) * per_layer)]
    state = {'next': 0, 'under_way': 0, 'free_chunks': SLOTS, 'free_qkv': 1}
    size_of = {'qkv': QKV_CHUNKS, 'cache': CACHE_CHUNKS, 'chunk': 1}

    def fill(limit):
        while state['next'] < len(queue):
            kind, index = queue[state['next']]
            if state['under_way'] and state['under_way'] + size_of[kind] > limit:
                return
            if kind == 'qkv':
                if index >= state['free_qkv']:
                    return
                for j in range(QKV_PARTS):
                    for copy in qkv_copies(index, j):
                        copy.start()
            elif kind == 'cache':
                for copy in cache_copies(index):
                    copy.start()
            else:
                if index >= state['free_chunks']:
                    return
                for copy in chunk_copies(*chunk_of(index), index % SLOTS):
                    copy.start()
            state['under_way'] += size_of[kind]
            state['next'] += 1

    def stream_dot(lhs_ref, layer, first, groups):
        out = jnp.zeros(acc.shape, F32)
        row = 0
        c = layer * per_layer + first
        for group in groups:
            members = range(c, c + group)
            for i in members:
                for copy in chunk_copies(*chunk_of(i), i % SLOTS):
                    copy.wait()
            state['under_way'] -= group
            fill(WINDOW)
            for i in members:
                n = dn_rest if chunk_of(i)[0] == 'rest' else CHUNK
                out = out + jnp.dot(lhs_ref[:, pl.ds(row, n)], ring[i % SLOTS, pl.ds(0, n)], preferred_element_type=F32)
                row += n
            state['free_chunks'] += group
            c += group
        acc[...] = out
        fill(WINDOW)

    qkv_rows = width // QKV_PARTS

    def qkv_copies(layer, j):
        piece = pl.ds(j * qkv_rows, qkv_rows)
        return [pltpu.make_async_copy(src.at[layer, piece], dst.at[piece], qkv_sem.at[i, j])
                for i, (src, dst) in enumerate(((wq, bq), (wk, bk), (wv, bv)))]

    def cache_copies(layer):
        pairs = ((kl_in, kl), (vl_in, vl)) if layer == 0 else ((kg_in, kg), (vg_in, vg))
        return [pltpu.make_async_copy(src.at[b], dst.at[b], cache_sem.at[layer, i, b])
                for i, (src, dst) in enumerate(pairs) for b in range(rows)]

    def send_copies(phase):
        copies = []
        for step in range(1, n_tp):
            peer = lax.rem(me + step, n_tp)
            copies.append(pltpu.make_async_remote_copy(
                src_ref=part.at[phase, me], dst_ref=part.at[phase, me],
                send_sem=send_sem.at[phase, step - 1], recv_sem=recv_sem.at[phase, step - 1],
                device_id={'tp': peer}, device_id_type=MESH))
        return copies

    def exchange(phase, meanwhile=None):
        part[phase, me] = acc[...].astype(BF16)
        copies = send_copies(phase)
        for copy in copies:
            copy.start()
        fill(SUM_WINDOW)
        if meanwhile is not None:
            meanwhile()
        for copy in copies:
            copy.wait_recv()
        total = part[phase, 0].astype(F32)
        for j in range(1, n_tp):
            total = total + part[phase, j].astype(F32)
        return total

    def gain(layer, i):
        return norm_ref[layer, pl.ds(i, 1), :]

    def add_normed(layer, i, branch_sum):
        x = (x_ref[...] + rms_norm(branch_sum, gain(layer, i)).astype(F32)).astype(BF16)
        x_ref[...] = x.astype(F32)
        return x

    def rotate(values, trig):
        first, second = values[:, :half], values[:, half:]
        cos_part, sin_part = trig
        return jnp.concatenate([first * cos_part - second * sin_part, second * cos_part + first * sin_part], axis=-1)

    def store_row(cache, b, slot, new_row):
        n = cache.shape[1]
        step = min(n, KV_STEP)

        def body(i, carry):
            piece = pl.ds(pl.multiple_of(i * step, step), step)
            ids = lax.broadcasted_iota(jnp.int32, (step, head), 0) + i * step
            cache[b, piece] = jnp.where(ids == slot, jnp.broadcast_to(new_row, (step, head)), cache[b, piece])
            return carry

        lax.fori_loop(0, n // step, body, 0)

    def attention(layer, kc, vc, trig):
        n = kc.shape[1]
        a_ref[...] = rms_norm(x_ref[...], gain(layer, 0))
        hq = bq.shape[1]

        q, k, v = jnp.zeros((rows, hq), F32), jnp.zeros((rows, head), F32), jnp.zeros((rows, head), F32)
        if layer > 0:
            for j in range(QKV_PARTS):
                for copy in qkv_copies(layer, j):
                    copy.wait()
        for j in range(QKV_PARTS):
            if layer == 0:
                for copy in qkv_copies(layer, j):
                    copy.wait()
            piece = pl.ds(j * qkv_rows, qkv_rows)
            lhs = a_ref[:, piece]
            q = q + jnp.dot(lhs, bq[piece], preferred_element_type=F32)
            k = k + jnp.dot(lhs, bk[piece], preferred_element_type=F32)
            v = v + jnp.dot(lhs, bv[piece], preferred_element_type=F32)
        state['under_way'] -= QKV_CHUNKS
        state['free_qkv'] += 1
        fill(WINDOW)
        group = hq // head
        queries = jnp.concatenate([rotate(q[:, g * head:(g + 1) * head], trig) for g in range(group)], axis=0).astype(BF16)
        k_new = rotate(k, trig).astype(BF16)
        v_new = v.astype(BF16)
        for copy in cache_copies(layer):
            copy.wait()
        state['under_way'] -= CACHE_CHUNKS
        fill(WINDOW)
        q_rows = group * rows
        row_seq = lax.rem(lax.broadcasted_iota(jnp.int32, (q_rows, 1), 0), rows)
        last, slot = jnp.zeros((q_rows, 1), jnp.int32), jnp.zeros((q_rows, 1), jnp.int32)
        for b in range(rows):
            last = jnp.where(row_seq == b, pos_ref[b], last)
            slot = jnp.where(row_seq == b, lax.rem(pos_ref[b], n), slot)

        def pick(per_seq):
            out = per_seq[0]
            for b in range(1, rows):
                out = jnp.where(row_seq == b, per_seq[b], out)
            return out

        step = min(n, KV_STEP)
        contract_last = (((1,), (1,)), ((), ()))

        def soft_exp(s):
            return jnp.exp(SOFT_CAP * jnp.tanh(s * head ** -0.5 / SOFT_CAP))

        per_row = [jnp.concatenate([new.astype(F32)] * group, axis=0) for new in (k_new, v_new)]
        e_new = soft_exp(jnp.sum(queries.astype(F32) * per_row[0], axis=-1, keepdims=True))
        total = e_new
        weights = []
        for i in range(n // step):
            piece = pl.ds(i * step, step)
            s = pick([lax.dot_general(queries, kc[b, piece], contract_last, preferred_element_type=F32) for b in range(rows)])
            ids = lax.broadcasted_iota(jnp.int32, (q_rows, step), 1) + i * step
            e = jnp.where((ids <= last) & (ids != slot), soft_exp(s), 0.0)
            e_ref[:, piece] = e
            total = total + jnp.sum(e, axis=-1, keepdims=True)
        out = (e_new / total).astype(BF16).astype(F32) * per_row[1]
        for i in range(n // step):
            piece = pl.ds(i * step, step)
            probs = (e_ref[:, piece] / total).astype(BF16)
            out = out + pick([jnp.dot(probs, vc[b, piece], preferred_element_type=F32) for b in range(rows)])
        mixed = out.astype(BF16)
        for g in range(group):
            o_ref[:, pl.ds(g * head, head)] = mixed[g * rows:(g + 1) * rows]

        def store_new():
            for b in range(rows):
                store_row(kc, b, lax.rem(pos_ref[b], n), k_new[b:b + 1])
                store_row(vc, b, lax.rem(pos_ref[b], n), v_new[b:b + 1])

        return store_new

    small = [pltpu.make_async_copy(src, dst, small_sem.at[i]) for i, (src, dst) in enumerate(
        ((hid_in, hid_ref), (norm_in, norm_ref), (pos_in, pos_ref), (freq_in, freq_ref)))]
    for copy in small:
        copy.start()
    fill(START_WINDOW)

    barrier = pltpu.get_barrier_semaphore()
    for step in range(1, n_tp):
        pl.semaphore_signal(barrier, inc=1, device_id={'tp': lax.rem(me + step, n_tp)}, device_id_type=MESH)

    for copy in small:
        copy.wait()
    x_ref[...] = hid_ref[...].astype(F32)
    row_ids = lax.broadcasted_iota(jnp.int32, (rows, half), 0)
    pos_rows = jnp.zeros((rows, half), F32)
    for b in range(rows):
        pos_rows = jnp.where(row_ids == b, pos_ref[b].astype(F32), pos_rows)
    angles = pos_rows * freq_ref[...]
    trig = jnp.cos(angles), jnp.sin(angles)
    for layer in range(layers):
        kc, vc = (kl, vl) if layer == 0 else (kg, vg)
        store_new = attention(layer, kc, vc, trig)
        stream_dot(o_ref, layer, 0, (n_wo,))
        if layer == 0:
            pl.semaphore_wait(barrier, n_tp - 1)
        x = add_normed(layer, 1, exchange(2 * layer, store_new))
        a_ref[...] = rms_norm(x.astype(F32), gain(layer, 2))
        stream_dot(a_ref, layer, at_gu, split(n_gu, GU_GROUP))
        gate_up = acc[...]
        h_ref[...] = (jax.nn.gelu(gate_up[:, :ff], approximate=True) * gate_up[:, ff:]).astype(BF16)
        stream_dot(h_ref, layer, at_dn, split(per_layer - at_dn, DN_GROUP))
        x = add_normed(layer, 3, exchange(2 * layer + 1))
    hid_out[...] = x
    for phase in range(2 * layers):
        for copy in send_copies(phase):
            copy.wait_send()


def write_kernel(*refs):
    n = len(refs) // 2
    copies = [pltpu.make_async_copy(refs[i], refs[n + i], refs[-1].at[i]) for i in range(n)]
    for copy in copies:
        copy.start()
    for copy in copies:
        copy.wait()


def decode_step(n_tp, hidden, positions, k_local, v_local, k_global, v_global, w_query, w_key, w_value, w_out, w_gate, w_up, w_down, norm_scale):
    rows, width = hidden.shape
    caches = [c.reshape(c.shape[0], c.shape[1], c.shape[3]) for c in (k_local, v_local, k_global, v_global)]
    head = caches[0].shape[2]
    half = head // 2
    inv_freq = jnp.asarray(ROPE_BASE ** (-2.0 * np.arange(half) / head), F32)[None, :]
    hq, ff, layers = w_query.shape[2], w_gate.shape[2], w_gate.shape[0]
    n_ctx = max(c.shape[1] for c in caches)
    vmem = pl.BlockSpec(memory_space=pltpu.VMEM)
    hbm = pl.BlockSpec(memory_space=pl.ANY)
    outs = pl.pallas_call(
        functools.partial(step_kernel, n_tp),
        out_shape=tuple(pltpu.VMEM(a.shape, BF16) for a in (hidden, *caches)),
        in_specs=[hbm] * 15,
        out_specs=(vmem,) * 5,
        scratch_shapes=[
            pltpu.SMEM((rows,), jnp.int32),
            pltpu.VMEM((rows, width), BF16),
            pltpu.VMEM((1, half), F32),
            pltpu.VMEM(norm_scale.shape, F32),
            pltpu.VMEM((SLOTS, CHUNK, width), BF16),
            pltpu.VMEM((width, hq), BF16),
            pltpu.VMEM((width, head), BF16),
            pltpu.VMEM((width, head), BF16),
            pltpu.VMEM((rows, width), F32),
            pltpu.VMEM((rows, width), BF16),
            pltpu.VMEM((rows, hq), BF16),
            pltpu.VMEM((rows, ff), BF16),
            pltpu.VMEM((rows, 2 * ff), F32),
            pltpu.VMEM((hq // head * rows, n_ctx), F32),
            pltpu.VMEM((2 * layers, n_tp, rows, width), BF16),
            pltpu.SemaphoreType.DMA((4,)),
            pltpu.SemaphoreType.DMA((SLOTS, 2)),
            pltpu.SemaphoreType.DMA((3, QKV_PARTS)),
            pltpu.SemaphoreType.DMA((2, 2, rows)),
            pltpu.SemaphoreType.DMA((2 * layers, n_tp - 1)),
            pltpu.SemaphoreType.DMA((2 * layers, n_tp - 1)),
        ],
        compiler_params=pltpu.CompilerParams(
            collective_id=0, has_side_effects=True, vmem_limit_bytes=VMEM_LIMIT),
        name='decode_step',
    )(positions, hidden, inv_freq, norm_scale, *caches, w_query, w_key, w_value, w_out, w_gate, w_up, w_down)
    hidden_out, *new_caches = pl.pallas_call(
        write_kernel,
        out_shape=tuple(jax.ShapeDtypeStruct(o.shape, o.dtype) for o in outs),
        in_specs=[hbm] * len(outs),
        out_specs=(hbm,) * len(outs),
        scratch_shapes=[pltpu.SemaphoreType.DMA((len(outs),))],
        compiler_params=pltpu.CompilerParams(vmem_limit_bytes=1024 * 1024),
        name='write_out',
    )(*outs)
    new_caches = [c.reshape(old.shape) for c, old in zip(new_caches, (k_local, v_local, k_global, v_global))]
    return (hidden_out, *new_caches)


def solution(mesh):
    row_spec = P('dp', None)
    cache_spec = P('dp', None, 'tp', None)
    col_split = P(None, None, 'tp')
    row_split = P(None, 'tp', None)
    in_specs = (row_spec, P('dp'), cache_spec, cache_spec, cache_spec, cache_spec, col_split, col_split, col_split, row_split, col_split, col_split, row_split, P())
    out_specs = (row_spec, cache_spec, cache_spec, cache_spec, cache_spec)
    return jax.shard_map(functools.partial(decode_step, mesh.shape['tp']), mesh=mesh, in_specs=in_specs, out_specs=out_specs, check_vma=False)
```

```python
import functools

import jax
import jax.numpy as jnp
import numpy as np
from jax import lax
from jax.experimental import pallas as pl
from jax.experimental.pallas import tpu as pltpu
from jax.sharding import PartitionSpec as P

SOFT_CAP = 50.0
NORM_EPS = 1e-6
ROPE_BASE = 10000.0

CHUNK = 256
SLOTS = 22
QKV_PARTS = 5
KV_STEP = 2048
GU_GROUP = 5
DN_GROUP = 3
QKV_CHUNKS, CACHE_CHUNKS = 4, 3
START_WINDOW, WINDOW, SUM_WINDOW = 10, 8, 20

VMEM_LIMIT = 52 * 1024 * 1024

F32 = jnp.float32
BF16 = jnp.bfloat16
MESH = pl.DeviceIdType.MESH


def rem(a, b):
    return a % b if isinstance(a, int) else lax.rem(a, b)


def split(count, group):
    return [min(group, count - i) for i in range(0, count, group)]


def rms_norm(values, gain_row):
    inv_rms = lax.rsqrt(jnp.mean(values * values, axis=-1, keepdims=True) + NORM_EPS)
    return (values * inv_rms * (1.0 + gain_row)).astype(BF16)


def step_kernel(n_tp, pos_in, hid_in, freq_in, norm_in, kl_in, vl_in, kg_in, vg_in, wq, wk, wv, wo, wg, wu, wd,
                hid_out, kl, vl, kg, vg,
                pos_ref, hid_ref, freq_ref, norm_ref, ring, bq, bk, bv, x_ref, a_ref, o_ref, h_ref, acc, e_ref, part,
                small_sem, ring_sem, qkv_sem, cache_sem, send_sem, recv_sem):
    rows, width = hid_ref.shape
    head = kl.shape[2]
    half = head // 2
    ff = wg.shape[2]
    layers = wg.shape[0]
    n_wo = wo.shape[1] // CHUNK
    n_gu = width // CHUNK
    n_dn = ff // CHUNK
    dn_rest = ff - n_dn * CHUNK
    at_gu, at_dn = n_wo, n_wo + n_gu
    per_layer = n_wo + n_gu + n_dn + (1 if dn_rest else 0)
    me = lax.axis_index('tp')

    def chunk_copies(kind, layer, k, slot):
        if kind == 'wo':
            return [pltpu.make_async_copy(wo.at[layer, pl.ds(k * CHUNK, CHUNK)], ring.at[slot], ring_sem.at[slot, 0])]
        if kind == 'gu':
            return [
                pltpu.make_async_copy(wg.at[layer, pl.ds(k * CHUNK, CHUNK)], ring.at[slot, :, pl.ds(0, ff)], ring_sem.at[slot, 0]),
                pltpu.make_async_copy(wu.at[layer, pl.ds(k * CHUNK, CHUNK)], ring.at[slot, :, pl.ds(ff, ff)], ring_sem.at[slot, 1]),
            ]
        if kind == 'dn':
            return [pltpu.make_async_copy(wd.at[layer, pl.ds(k * CHUNK, CHUNK)], ring.at[slot], ring_sem.at[slot, 0])]
        return [pltpu.make_async_copy(wd.at[layer, pl.ds(n_dn * CHUNK, dn_rest)], ring.at[slot, pl.ds(0, dn_rest)], ring_sem.at[slot, 0])]

    def chunk_of(c):
        layer, r = divmod(c, per_layer)
        if r < at_gu:
            return 'wo', layer, r
        if r < at_dn:
            return 'gu', layer, r - at_gu
        if r < at_dn + n_dn:
            return 'dn', layer, r - at_dn
        return 'rest', layer, 0

    queue = []
    for layer in range(layers):
        queue += [('qkv', layer), ('cache', layer)]
        queue += [('chunk', c) for c in range(layer * per_layer, (layer + 1) * per_layer)]
    state = {'next': 0, 'under_way': 0, 'free_chunks': SLOTS, 'free_qkv': 1}
    size_of = {'qkv': QKV_CHUNKS, 'cache': CACHE_CHUNKS, 'chunk': 1}

    def started(*item):
        assert queue.index(item) < state['next'], item

    def fill(limit, stop=None):
        while state['next'] < len(queue) and queue[state['next']] != stop:
            kind, index = queue[state['next']]
            if state['under_way'] and state['under_way'] + size_of[kind] > limit:
                return
            if kind == 'qkv':
                if index >= state['free_qkv']:
                    return
                for j in range(QKV_PARTS):
                    for copy in qkv_copies(index, j):
                        copy.start()
            elif kind == 'cache':
                for copy in cache_copies(index):
                    copy.start()
            else:
                if index >= state['free_chunks']:
                    return
                for copy in chunk_copies(*chunk_of(index), index % SLOTS):
                    copy.start()
            state['under_way'] += size_of[kind]
            state['next'] += 1

    def stream_dot(lhs_ref, layer, first, groups):
        out = jnp.zeros(acc.shape, F32)
        row = 0
        c = layer * per_layer + first
        for group in groups:
            members = range(c, c + group)
            for i in members:
                started('chunk', i)
                for copy in chunk_copies(*chunk_of(i), i % SLOTS):
                    copy.wait()
            state['under_way'] -= group
            fill(WINDOW)
            for i in members:
                n = dn_rest if chunk_of(i)[0] == 'rest' else CHUNK
                out = out + jnp.dot(lhs_ref[:, pl.ds(row, n)], ring[i % SLOTS, pl.ds(0, n)], preferred_element_type=F32)
                row += n
            state['free_chunks'] += group
            c += group
        acc[...] = out
        fill(WINDOW)

    def stream_loop(lhs_ref, layer, first, kind, steps, group, in_loop):
        base = layer * per_layer + first
        acc[...] = jnp.zeros_like(acc)
        ahead = 0
        if state['next'] < len(queue) and queue[state['next']] == ('chunk', base + steps * group):
            ahead = min(in_loop, n_dn // steps)
        for _ in range(ahead * steps):
            assert chunk_of(queue[state['next']][1])[0] == 'dn' and queue[state['next']][1] < base + SLOTS
            state['next'] += 1
            state['under_way'] += 1

        started('chunk', base + steps * group - 1)

        def body(i, carry):
            members = [(i * group + j, rem(base + i * group + j, SLOTS)) for j in range(group)]
            for k, slot in members:
                for copy in chunk_copies(kind, layer, k, slot):
                    copy.wait()
            for j in range(ahead):
                for copy in chunk_copies('dn', layer, i * ahead + j, rem(base + steps * group + i * ahead + j, SLOTS)):
                    copy.start()
            out = acc[...]
            for k, slot in members:
                lhs = lhs_ref[:, pl.ds(pl.multiple_of(k * CHUNK, CHUNK), CHUNK)]
                out = out + jnp.dot(lhs, ring[slot], preferred_element_type=F32)
            acc[...] = out
            return carry

        lax.fori_loop(0, steps, body, 0)
        state['under_way'] -= steps * group
        state['free_chunks'] += steps * group
        fill(WINDOW)

    qkv_rows = width // QKV_PARTS

    def qkv_copies(layer, j):
        piece = pl.ds(j * qkv_rows, qkv_rows)
        return [pltpu.make_async_copy(src.at[layer, piece], dst.at[piece], qkv_sem.at[i, j])
                for i, (src, dst) in enumerate(((wq, bq), (wk, bk), (wv, bv)))]

    def cache_copies(layer):
        pairs = ((kl_in, kl), (vl_in, vl)) if layer == 0 else ((kg_in, kg), (vg_in, vg))
        return [pltpu.make_async_copy(src.at[b], dst.at[b], cache_sem.at[layer, i, b])
                for i, (src, dst) in enumerate(pairs) for b in range(rows)]

    def send_copies(phase):
        copies = []
        for step in range(1, n_tp):
            peer = lax.rem(me + step, n_tp)
            copies.append(pltpu.make_async_remote_copy(
                src_ref=part.at[phase, me], dst_ref=part.at[phase, me],
                send_sem=send_sem.at[phase, step - 1], recv_sem=recv_sem.at[phase, step - 1],
                device_id={'tp': peer}, device_id_type=MESH))
        return copies

    def exchange(phase, limit, stop=None, meanwhile=None):
        part[phase, me] = acc[...].astype(BF16)
        copies = send_copies(phase)
        for copy in copies:
            copy.start()
        fill(limit, stop)
        if meanwhile is not None:
            meanwhile()
        for copy in copies:
            copy.wait_recv()
        total = part[phase, 0].astype(F32)
        for j in range(1, n_tp):
            total = total + part[phase, j].astype(F32)
        return total

    def gain(layer, i):
        return norm_ref[layer, pl.ds(i, 1), :]

    def add_normed(layer, i, branch_sum):
        x = (x_ref[...] + rms_norm(branch_sum, gain(layer, i)).astype(F32)).astype(BF16)
        x_ref[...] = x.astype(F32)
        return x

    def rotate(values, trig):
        first, second = values[:, :half], values[:, half:]
        cos_part, sin_part = trig
        return jnp.concatenate([first * cos_part - second * sin_part, second * cos_part + first * sin_part], axis=-1)

    def store_row(cache, b, slot, new_row):
        n = cache.shape[1]
        step = min(n, KV_STEP)

        def body(i, carry):
            piece = pl.ds(pl.multiple_of(i * step, step), step)
            ids = lax.broadcasted_iota(jnp.int32, (step, head), 0) + i * step
            cache[b, piece] = jnp.where(ids == slot, jnp.broadcast_to(new_row, (step, head)), cache[b, piece])
            return carry

        lax.fori_loop(0, n // step, body, 0)

    def attention(layer, kc, vc, trig):
        n = kc.shape[1]
        a_ref[...] = rms_norm(x_ref[...], gain(layer, 0))
        hq = bq.shape[1]

        started('qkv', layer)

        def qkv_body(j, carry):
            q, k, v = carry
            for copy in qkv_copies(layer, j):
                copy.wait()
            piece = pl.ds(pl.multiple_of(j * qkv_rows, qkv_rows), qkv_rows)
            lhs = a_ref[:, piece]
            q = q + jnp.dot(lhs, bq[piece], preferred_element_type=F32)
            k = k + jnp.dot(lhs, bk[piece], preferred_element_type=F32)
            v = v + jnp.dot(lhs, bv[piece], preferred_element_type=F32)
            return q, k, v

        q, k, v = lax.fori_loop(0, QKV_PARTS, qkv_body, (
            jnp.zeros((rows, hq), F32), jnp.zeros((rows, head), F32), jnp.zeros((rows, head), F32)))
        state['under_way'] -= QKV_CHUNKS
        state['free_qkv'] += 1
        fill(WINDOW)
        group = hq // head
        queries = jnp.concatenate([rotate(q[:, g * head:(g + 1) * head], trig) for g in range(group)], axis=0).astype(BF16)
        k_new = rotate(k, trig).astype(BF16)
        v_new = v.astype(BF16)
        started('cache', layer)
        for copy in cache_copies(layer):
            copy.wait()
        state['under_way'] -= CACHE_CHUNKS
        fill(WINDOW)
        q_rows = group * rows
        row_seq = lax.rem(lax.broadcasted_iota(jnp.int32, (q_rows, 1), 0), rows)
        last, slot = jnp.zeros((q_rows, 1), jnp.int32), jnp.zeros((q_rows, 1), jnp.int32)
        for b in range(rows):
            last = jnp.where(row_seq == b, pos_ref[b], last)
            slot = jnp.where(row_seq == b, lax.rem(pos_ref[b], n), slot)

        def pick(per_seq):
            out = per_seq[0]
            for b in range(1, rows):
                out = jnp.where(row_seq == b, per_seq[b], out)
            return out

        step = min(n, KV_STEP)
        contract_last = (((1,), (1,)), ((), ()))

        def soft_exp(s):
            return jnp.exp(SOFT_CAP * jnp.tanh(s * head ** -0.5 / SOFT_CAP))

        per_row = [jnp.concatenate([new.astype(F32)] * group, axis=0) for new in (k_new, v_new)]
        e_new = soft_exp(jnp.sum(queries.astype(F32) * per_row[0], axis=-1, keepdims=True))
        total = e_new
        def score_body(i, total):
            piece = pl.ds(pl.multiple_of(i * step, step), step)
            s = pick([lax.dot_general(queries, kc[b, piece], contract_last, preferred_element_type=F32) for b in range(rows)])
            ids = lax.broadcasted_iota(jnp.int32, (q_rows, step), 1) + i * step
            e = jnp.where((ids <= last) & (ids != slot), soft_exp(s), 0.0)
            e_ref[:, piece] = e
            return total + jnp.sum(e, axis=-1, keepdims=True)

        total = lax.fori_loop(0, n // step, score_body, total)

        def value_body(i, out):
            piece = pl.ds(pl.multiple_of(i * step, step), step)
            probs = (e_ref[:, piece] / total).astype(BF16)
            return out + pick([jnp.dot(probs, vc[b, piece], preferred_element_type=F32) for b in range(rows)])

        out = (e_new / total).astype(BF16).astype(F32) * per_row[1]
        out = lax.fori_loop(0, n // step, value_body, out)
        mixed = out.astype(BF16)
        for g in range(group):
            o_ref[:, pl.ds(g * head, head)] = mixed[g * rows:(g + 1) * rows]

        def store_new():
            for b in range(rows):
                store_row(kc, b, lax.rem(pos_ref[b], n), k_new[b:b + 1])
                store_row(vc, b, lax.rem(pos_ref[b], n), v_new[b:b + 1])

        return store_new

    small = [pltpu.make_async_copy(src, dst, small_sem.at[i]) for i, (src, dst) in enumerate(
        ((hid_in, hid_ref), (norm_in, norm_ref), (pos_in, pos_ref), (freq_in, freq_ref)))]
    for copy in small:
        copy.start()
    fill(START_WINDOW)

    barrier = pltpu.get_barrier_semaphore()
    for step in range(1, n_tp):
        pl.semaphore_signal(barrier, inc=1, device_id={'tp': lax.rem(me + step, n_tp)}, device_id_type=MESH)

    for copy in small:
        copy.wait()
    x_ref[...] = hid_ref[...].astype(F32)
    row_ids = lax.broadcasted_iota(jnp.int32, (rows, half), 0)
    pos_rows = jnp.zeros((rows, half), F32)
    for b in range(rows):
        pos_rows = jnp.where(row_ids == b, pos_ref[b].astype(F32), pos_rows)
    angles = pos_rows * freq_ref[...]
    trig = jnp.cos(angles), jnp.sin(angles)
    for layer in range(layers):
        kc, vc = (kl, vl) if layer == 0 else (kg, vg)
        store_new = attention(layer, kc, vc, trig)
        stream_dot(o_ref, layer, 0, (n_wo,))
        if layer == 0:
            pl.semaphore_wait(barrier, n_tp - 1)
        x = add_normed(layer, 1, exchange(2 * layer, len(queue) * QKV_CHUNKS, ('chunk', at_dn), store_new))
        a_ref[...] = rms_norm(x.astype(F32), gain(layer, 2))
        stream_loop(a_ref, layer, at_gu, 'gu', n_gu // GU_GROUP, GU_GROUP, 2)
        gate_up = acc[...]
        h_ref[...] = (jax.nn.gelu(gate_up[:, :ff], approximate=True) * gate_up[:, ff:]).astype(BF16)
        stream_dot(h_ref, layer, at_dn, split(per_layer - at_dn, DN_GROUP))
        x = add_normed(layer, 3, exchange(2 * layer + 1, SUM_WINDOW))
    hid_out[...] = x
    for phase in range(2 * layers):
        for copy in send_copies(phase):
            copy.wait_send()


def write_kernel(*refs):
    n = len(refs) // 2
    copies = [pltpu.make_async_copy(refs[i], refs[n + i], refs[-1].at[i]) for i in range(n)]
    for copy in copies:
        copy.start()
    for copy in copies:
        copy.wait()


def decode_step(n_tp, hidden, positions, k_local, v_local, k_global, v_global, w_query, w_key, w_value, w_out, w_gate, w_up, w_down, norm_scale):
    rows, width = hidden.shape
    caches = [c.reshape(c.shape[0], c.shape[1], c.shape[3]) for c in (k_local, v_local, k_global, v_global)]
    head = caches[0].shape[2]
    half = head // 2
    inv_freq = jnp.asarray(ROPE_BASE ** (-2.0 * np.arange(half) / head), F32)[None, :]
    hq, ff, layers = w_query.shape[2], w_gate.shape[2], w_gate.shape[0]
    n_ctx = max(c.shape[1] for c in caches)
    vmem = pl.BlockSpec(memory_space=pltpu.VMEM)
    hbm = pl.BlockSpec(memory_space=pl.ANY)
    outs = pl.pallas_call(
        functools.partial(step_kernel, n_tp),
        out_shape=tuple(pltpu.VMEM(a.shape, BF16) for a in (hidden, *caches)),
        in_specs=[hbm] * 15,
        out_specs=(vmem,) * 5,
        scratch_shapes=[
            pltpu.SMEM((rows,), jnp.int32),
            pltpu.VMEM((rows, width), BF16),
            pltpu.VMEM((1, half), F32),
            pltpu.VMEM(norm_scale.shape, F32),
            pltpu.VMEM((SLOTS, CHUNK, width), BF16),
            pltpu.VMEM((width, hq), BF16),
            pltpu.VMEM((width, head), BF16),
            pltpu.VMEM((width, head), BF16),
            pltpu.VMEM((rows, width), F32),
            pltpu.VMEM((rows, width), BF16),
            pltpu.VMEM((rows, hq), BF16),
            pltpu.VMEM((rows, ff), BF16),
            pltpu.VMEM((rows, 2 * ff), F32),
            pltpu.VMEM((hq // head * rows, n_ctx), F32),
            pltpu.VMEM((2 * layers, n_tp, rows, width), BF16),
            pltpu.SemaphoreType.DMA((4,)),
            pltpu.SemaphoreType.DMA((SLOTS, 2)),
            pltpu.SemaphoreType.DMA((3, QKV_PARTS)),
            pltpu.SemaphoreType.DMA((2, 2, rows)),
            pltpu.SemaphoreType.DMA((2 * layers, n_tp - 1)),
            pltpu.SemaphoreType.DMA((2 * layers, n_tp - 1)),
        ],
        compiler_params=pltpu.CompilerParams(
            collective_id=0, has_side_effects=True, vmem_limit_bytes=VMEM_LIMIT),
        name='decode_step',
    )(positions, hidden, inv_freq, norm_scale, *caches, w_query, w_key, w_value, w_out, w_gate, w_up, w_down)
    hidden_out, *new_caches = pl.pallas_call(
        write_kernel,
        out_shape=tuple(jax.ShapeDtypeStruct(o.shape, o.dtype) for o in outs),
        in_specs=[hbm] * len(outs),
        out_specs=(hbm,) * len(outs),
        scratch_shapes=[pltpu.SemaphoreType.DMA((len(outs),))],
        compiler_params=pltpu.CompilerParams(vmem_limit_bytes=1024 * 1024),
        name='write_out',
    )(*outs)
    new_caches = [c.reshape(old.shape) for c, old in zip(new_caches, (k_local, v_local, k_global, v_global))]
    return (hidden_out, *new_caches)


def solution(mesh):
    row_spec = P('dp', None)
    cache_spec = P('dp', None, 'tp', None)
    col_split = P(None, None, 'tp')
    row_split = P(None, 'tp', None)
    in_specs = (row_spec, P('dp'), cache_spec, cache_spec, cache_spec, cache_spec, col_split, col_split, col_split, row_split, col_split, col_split, row_split, P())
    out_specs = (row_spec, cache_spec, cache_spec, cache_spec, cache_spec)
    return jax.shard_map(functools.partial(decode_step, mesh.shape['tp']), mesh=mesh, in_specs=in_specs, out_specs=out_specs, check_vma=False)
```

```python
import functools

import jax
import jax.numpy as jnp
import numpy as np
from jax import lax
from jax.experimental import pallas as pl
from jax.experimental.pallas import tpu as pltpu
from jax.sharding import PartitionSpec as P

SOFT_CAP = 50.0
NORM_EPS = 1e-6
ROPE_BASE = 10000.0

CHUNK = 256
SLOTS = 22
QKV_PARTS = 3
KV_STEP = 2048
GU_GROUP = 5
DN_GROUP = 3
QKV_CHUNKS, CACHE_CHUNKS = 4, 3
START_WINDOW, WINDOW, SUM_WINDOW = 10, 8, 20

VMEM_LIMIT = 52 * 1024 * 1024

F32 = jnp.float32
BF16 = jnp.bfloat16
MESH = pl.DeviceIdType.MESH


def rem(a, b):
    return a % b if isinstance(a, int) else lax.rem(a, b)


def split(count, group):
    return [min(group, count - i) for i in range(0, count, group)]


def rms_norm(values, gain_row):
    inv_rms = lax.rsqrt(jnp.mean(values * values, axis=-1, keepdims=True) + NORM_EPS)
    return (values * inv_rms * (1.0 + gain_row)).astype(BF16)


def step_kernel(n_tp, pos_in, hid_in, freq_in, norm_in, kl_in, vl_in, kg_in, vg_in, wq, wk, wv, wo, wg, wu, wd,
                hid_out, kl, vl, kg, vg,
                pos_ref, hid_ref, freq_ref, norm_ref, ring, bq, bk, bv, x_ref, a_ref, o_ref, h_ref, acc, e_ref, part,
                small_sem, ring_sem, qkv_sem, cache_sem, send_sem, recv_sem):
    rows, width = hid_ref.shape
    head = kl.shape[2]
    half = head // 2
    ff = wg.shape[2]
    layers = wg.shape[0]
    n_wo = wo.shape[1] // CHUNK
    n_gu = width // CHUNK
    n_dn = ff // CHUNK
    dn_rest = ff - n_dn * CHUNK
    at_gu, at_dn = n_wo, n_wo + n_gu
    per_layer = n_wo + n_gu + n_dn + (1 if dn_rest else 0)
    me = lax.axis_index('tp')
    cut = pl.cdiv(width, 2 * CHUNK) * CHUNK
    pieces = ((0, cut), (cut, width - cut))

    def chunk_copies(kind, layer, k, slot):
        if kind == 'wo':
            return [pltpu.make_async_copy(wo.at[layer, pl.ds(k * CHUNK, CHUNK)], ring.at[slot], ring_sem.at[slot, 0])]
        if kind == 'gu':
            return [
                pltpu.make_async_copy(wg.at[layer, pl.ds(k * CHUNK, CHUNK)], ring.at[slot, :, pl.ds(0, ff)], ring_sem.at[slot, 0]),
                pltpu.make_async_copy(wu.at[layer, pl.ds(k * CHUNK, CHUNK)], ring.at[slot, :, pl.ds(ff, ff)], ring_sem.at[slot, 1]),
            ]
        if kind == 'dn':
            return [pltpu.make_async_copy(wd.at[layer, pl.ds(k * CHUNK, CHUNK)], ring.at[slot], ring_sem.at[slot, 0])]
        return [pltpu.make_async_copy(wd.at[layer, pl.ds(n_dn * CHUNK, dn_rest)], ring.at[slot, pl.ds(0, dn_rest)], ring_sem.at[slot, 0])]

    def chunk_of(c):
        layer, r = divmod(c, per_layer)
        if r < at_gu:
            return 'wo', layer, r
        if r < at_dn:
            return 'gu', layer, r - at_gu
        if r < at_dn + n_dn:
            return 'dn', layer, r - at_dn
        return 'rest', layer, 0

    queue = []
    for layer in range(layers):
        queue += [('qkv', layer), ('cache', layer)]
        queue += [('chunk', c) for c in range(layer * per_layer, (layer + 1) * per_layer)]
    state = {'next': 0, 'under_way': 0, 'free_chunks': SLOTS, 'free_qkv': 1}
    size_of = {'qkv': QKV_CHUNKS, 'cache': CACHE_CHUNKS, 'chunk': 1}

    def started(*item):
        assert queue.index(item) < state['next'], item

    def fill(limit, stop=None):
        while state['next'] < len(queue) and queue[state['next']] != stop:
            kind, index = queue[state['next']]
            if state['under_way'] and state['under_way'] + size_of[kind] > limit:
                return
            if kind == 'qkv':
                if index >= state['free_qkv']:
                    return
                for j in range(QKV_PARTS):
                    for copy in qkv_copies(index, j):
                        copy.start()
            elif kind == 'cache':
                for copy in cache_copies(index):
                    copy.start()
            else:
                if index >= state['free_chunks']:
                    return
                for copy in chunk_copies(*chunk_of(index), index % SLOTS):
                    copy.start()
            state['under_way'] += size_of[kind]
            state['next'] += 1

    def stream_dot(lhs_ref, layer, first, groups, phase):
        out = None
        row = 0
        c = layer * per_layer + first
        for g, group in enumerate(groups):
            members = range(c, c + group)
            for i in members:
                started('chunk', i)
                for copy in chunk_copies(*chunk_of(i), i % SLOTS):
                    copy.wait()
            state['under_way'] -= group
            fill(WINDOW)
            terms = []
            for i in members:
                n = dn_rest if chunk_of(i)[0] == 'rest' else CHUNK
                terms.append((lhs_ref[:, pl.ds(row, n)], i % SLOTS, n))
                row += n

            def product(columns):
                start, size = columns
                parts = [] if out is None else [out[:, start:start + size]]
                for lhs, slot, n in terms:
                    parts.append(jnp.dot(lhs, ring[slot, pl.ds(0, n), pl.ds(start, size)], preferred_element_type=F32))
                return functools.reduce(jnp.add, parts)

            state['free_chunks'] += group
            c += group
            if g < len(groups) - 1:
                out = product((0, width))
                continue
            for p, columns in enumerate(pieces):
                part[phase, me, :, pl.ds(*columns)] = product(columns).astype(BF16)
                for copy in send_copies(phase, p):
                    copy.start()

    def stream_loop(lhs_ref, layer, first, kind, steps, group, in_loop):
        base = layer * per_layer + first
        acc[...] = jnp.zeros_like(acc)
        ahead = 0
        if state['next'] < len(queue) and queue[state['next']] == ('chunk', base + steps * group):
            ahead = min(in_loop, n_dn // steps)
        for _ in range(ahead * steps):
            assert chunk_of(queue[state['next']][1])[0] == 'dn' and queue[state['next']][1] < base + SLOTS
            state['next'] += 1
            state['under_way'] += 1

        started('chunk', base + steps * group - 1)

        def body(i, carry):
            members = [(i * group + j, rem(base + i * group + j, SLOTS)) for j in range(group)]
            for k, slot in members:
                for copy in chunk_copies(kind, layer, k, slot):
                    copy.wait()
            for j in range(ahead):
                for copy in chunk_copies('dn', layer, i * ahead + j, rem(base + steps * group + i * ahead + j, SLOTS)):
                    copy.start()
            out = acc[...]
            for k, slot in members:
                lhs = lhs_ref[:, pl.ds(pl.multiple_of(k * CHUNK, CHUNK), CHUNK)]
                out = out + jnp.dot(lhs, ring[slot], preferred_element_type=F32)
            acc[...] = out
            return carry

        lax.fori_loop(0, steps, body, 0)
        state['under_way'] -= steps * group
        state['free_chunks'] += steps * group
        fill(WINDOW)

    qkv_rows = width // QKV_PARTS

    def qkv_copies(layer, j):
        piece = pl.ds(j * qkv_rows, qkv_rows)
        return [pltpu.make_async_copy(src.at[layer, piece], dst.at[piece], qkv_sem.at[i, j])
                for i, (src, dst) in enumerate(((wq, bq), (wk, bk), (wv, bv)))]

    def cache_copies(layer):
        pairs = ((kl_in, kl), (vl_in, vl)) if layer == 0 else ((kg_in, kg), (vg_in, vg))
        return [pltpu.make_async_copy(src.at[b], dst.at[b], cache_sem.at[layer, i, b])
                for i, (src, dst) in enumerate(pairs) for b in range(rows)]

    def send_copies(phase, p):
        copies = []
        for step in range(1, n_tp):
            peer = lax.rem(me + step, n_tp)
            mine = part.at[phase, me, :, pl.ds(*pieces[p])]
            copies.append(pltpu.make_async_remote_copy(
                src_ref=mine, dst_ref=mine,
                send_sem=send_sem.at[phase, p, step - 1], recv_sem=recv_sem.at[phase, p, step - 1],
                device_id={'tp': peer}, device_id_type=MESH))
        return copies

    def collect(phase, limit, stop=None, meanwhile=None):
        fill(limit, stop)
        if meanwhile is not None:
            meanwhile()
        sums = []
        for p, columns in enumerate(pieces):
            for copy in send_copies(phase, p):
                copy.wait_recv()
            total = part[phase, 0, :, pl.ds(*columns)].astype(F32)
            for j in range(1, n_tp):
                total = total + part[phase, j, :, pl.ds(*columns)].astype(F32)
            sums.append(total)
        return jnp.concatenate(sums, axis=-1)

    def gain(layer, i):
        return norm_ref[layer, pl.ds(i, 1), :]

    def add_normed(layer, i, branch_sum):
        x = (x_ref[...] + rms_norm(branch_sum, gain(layer, i)).astype(F32)).astype(BF16)
        x_ref[...] = x.astype(F32)
        return x

    def rotate(values, trig):
        first, second = values[:, :half], values[:, half:]
        cos_part, sin_part = trig
        return jnp.concatenate([first * cos_part - second * sin_part, second * cos_part + first * sin_part], axis=-1)

    def store_row(cache, b, slot, new_row):
        n = cache.shape[1]
        step = min(n, KV_STEP)

        def body(i, carry):
            piece = pl.ds(pl.multiple_of(i * step, step), step)
            ids = lax.broadcasted_iota(jnp.int32, (step, head), 0) + i * step
            cache[b, piece] = jnp.where(ids == slot, jnp.broadcast_to(new_row, (step, head)), cache[b, piece])
            return carry

        lax.fori_loop(0, n // step, body, 0)

    def attention(layer, kc, vc, trig):
        n = kc.shape[1]
        a_ref[...] = rms_norm(x_ref[...], gain(layer, 0))
        hq = bq.shape[1]

        started('qkv', layer)

        def qkv_body(j, carry):
            q, k, v = carry
            for copy in qkv_copies(layer, j):
                copy.wait()
            piece = pl.ds(pl.multiple_of(j * qkv_rows, qkv_rows), qkv_rows)
            lhs = a_ref[:, piece]
            q = q + jnp.dot(lhs, bq[piece], preferred_element_type=F32)
            k = k + jnp.dot(lhs, bk[piece], preferred_element_type=F32)
            v = v + jnp.dot(lhs, bv[piece], preferred_element_type=F32)
            return q, k, v

        q, k, v = lax.fori_loop(0, QKV_PARTS, qkv_body, (
            jnp.zeros((rows, hq), F32), jnp.zeros((rows, head), F32), jnp.zeros((rows, head), F32)))
        state['under_way'] -= QKV_CHUNKS
        state['free_qkv'] += 1
        fill(WINDOW)
        group = hq // head
        queries = jnp.concatenate([rotate(q[:, g * head:(g + 1) * head], trig) for g in range(group)], axis=0).astype(BF16)
        k_new = rotate(k, trig).astype(BF16)
        v_new = v.astype(BF16)
        started('cache', layer)
        for copy in cache_copies(layer):
            copy.wait()
        state['under_way'] -= CACHE_CHUNKS
        fill(WINDOW)
        q_rows = group * rows
        row_seq = lax.rem(lax.broadcasted_iota(jnp.int32, (q_rows, 1), 0), rows)
        last, slot = jnp.zeros((q_rows, 1), jnp.int32), jnp.zeros((q_rows, 1), jnp.int32)
        for b in range(rows):
            last = jnp.where(row_seq == b, pos_ref[b], last)
            slot = jnp.where(row_seq == b, lax.rem(pos_ref[b], n), slot)

        def pick(per_seq):
            out = per_seq[0]
            for b in range(1, rows):
                out = jnp.where(row_seq == b, per_seq[b], out)
            return out

        step = min(n, KV_STEP)
        contract_last = (((1,), (1,)), ((), ()))

        def soft_exp(s):
            return jnp.exp(SOFT_CAP * jnp.tanh(s * (head ** -0.5 / SOFT_CAP)))

        per_row = [jnp.concatenate([new.astype(F32)] * group, axis=0) for new in (k_new, v_new)]
        e_new = soft_exp(jnp.sum(queries.astype(F32) * per_row[0], axis=-1, keepdims=True))
        total = e_new
        def score_body(i, total):
            piece = pl.ds(pl.multiple_of(i * step, step), step)
            s = pick([lax.dot_general(queries, kc[b, piece], contract_last, preferred_element_type=F32) for b in range(rows)])
            ids = lax.broadcasted_iota(jnp.int32, (q_rows, step), 1) + i * step
            e = jnp.where((ids <= last) & (ids != slot), soft_exp(s), 0.0)
            e_ref[:, piece] = e
            return total + jnp.sum(e, axis=-1, keepdims=True)

        total = lax.fori_loop(0, n // step, score_body, total)

        def value_body(i, out):
            piece = pl.ds(pl.multiple_of(i * step, step), step)
            probs = (e_ref[:, piece] * inv_total).astype(BF16)
            return out + pick([jnp.dot(probs, vc[b, piece], preferred_element_type=F32) for b in range(rows)])

        inv_total = 1.0 / total
        out = (e_new * inv_total).astype(BF16).astype(F32) * per_row[1]
        out = lax.fori_loop(0, n // step, value_body, out)
        mixed = out.astype(BF16)
        for g in range(group):
            o_ref[:, pl.ds(g * head, head)] = mixed[g * rows:(g + 1) * rows]

        def store_new():
            for b in range(rows):
                store_row(kc, b, lax.rem(pos_ref[b], n), k_new[b:b + 1])
                store_row(vc, b, lax.rem(pos_ref[b], n), v_new[b:b + 1])

        return store_new

    small = [pltpu.make_async_copy(src, dst, small_sem.at[i]) for i, (src, dst) in enumerate(
        ((hid_in, hid_ref), (norm_in, norm_ref), (pos_in, pos_ref), (freq_in, freq_ref)))]
    for copy in small:
        copy.start()
    fill(START_WINDOW)

    barrier = pltpu.get_barrier_semaphore()
    for step in range(1, n_tp):
        pl.semaphore_signal(barrier, inc=1, device_id={'tp': lax.rem(me + step, n_tp)}, device_id_type=MESH)

    for copy in small:
        copy.wait()
    x_ref[...] = hid_ref[...].astype(F32)
    row_ids = lax.broadcasted_iota(jnp.int32, (rows, half), 0)
    pos_rows = jnp.zeros((rows, half), F32)
    for b in range(rows):
        pos_rows = jnp.where(row_ids == b, pos_ref[b].astype(F32), pos_rows)
    angles = pos_rows * freq_ref[...]
    trig = jnp.cos(angles), jnp.sin(angles)
    for layer in range(layers):
        kc, vc = (kl, vl) if layer == 0 else (kg, vg)
        store_new = attention(layer, kc, vc, trig)
        if layer == 0:
            pl.semaphore_wait(barrier, n_tp - 1)
        stream_dot(o_ref, layer, 0, (n_wo,), 2 * layer)
        x = add_normed(layer, 1, collect(2 * layer, len(queue) * QKV_CHUNKS, ('chunk', at_dn), store_new))
        a_ref[...] = rms_norm(x.astype(F32), gain(layer, 2))
        stream_loop(a_ref, layer, at_gu, 'gu', n_gu // GU_GROUP, GU_GROUP, 2)
        gate_up = acc[...]
        h_ref[...] = (jax.nn.gelu(gate_up[:, :ff], approximate=True) * gate_up[:, ff:]).astype(BF16)
        stream_dot(h_ref, layer, at_dn, split(per_layer - at_dn, DN_GROUP), 2 * layer + 1)
        x = add_normed(layer, 3, collect(2 * layer + 1, SUM_WINDOW))
    hid_out[...] = x
    for phase in range(2 * layers):
        for p in range(len(pieces)):
            for copy in send_copies(phase, p):
                copy.wait_send()


def write_kernel(*refs):
    n = len(refs) // 2
    copies = [pltpu.make_async_copy(refs[i], refs[n + i], refs[-1].at[i]) for i in range(n)]
    for copy in copies:
        copy.start()
    for copy in copies:
        copy.wait()


def decode_step(n_tp, hidden, positions, k_local, v_local, k_global, v_global, w_query, w_key, w_value, w_out, w_gate, w_up, w_down, norm_scale):
    rows, width = hidden.shape
    caches = [c.reshape(c.shape[0], c.shape[1], c.shape[3]) for c in (k_local, v_local, k_global, v_global)]
    head = caches[0].shape[2]
    half = head // 2
    inv_freq = jnp.asarray(ROPE_BASE ** (-2.0 * np.arange(half) / head), F32)[None, :]
    hq, ff, layers = w_query.shape[2], w_gate.shape[2], w_gate.shape[0]
    n_ctx = max(c.shape[1] for c in caches)
    vmem = pl.BlockSpec(memory_space=pltpu.VMEM)
    hbm = pl.BlockSpec(memory_space=pl.ANY)
    outs = pl.pallas_call(
        functools.partial(step_kernel, n_tp),
        out_shape=tuple(pltpu.VMEM(a.shape, BF16) for a in (hidden, *caches)),
        in_specs=[hbm] * 15,
        out_specs=(vmem,) * 5,
        scratch_shapes=[
            pltpu.SMEM((rows,), jnp.int32),
            pltpu.VMEM((rows, width), BF16),
            pltpu.VMEM((1, half), F32),
            pltpu.VMEM(norm_scale.shape, F32),
            pltpu.VMEM((SLOTS, CHUNK, width), BF16),
            pltpu.VMEM((width, hq), BF16),
            pltpu.VMEM((width, head), BF16),
            pltpu.VMEM((width, head), BF16),
            pltpu.VMEM((rows, width), F32),
            pltpu.VMEM((rows, width), BF16),
            pltpu.VMEM((rows, hq), BF16),
            pltpu.VMEM((rows, ff), BF16),
            pltpu.VMEM((rows, 2 * ff), F32),
            pltpu.VMEM((hq // head * rows, n_ctx), F32),
            pltpu.VMEM((2 * layers, n_tp, rows, width), BF16),
            pltpu.SemaphoreType.DMA((4,)),
            pltpu.SemaphoreType.DMA((SLOTS, 2)),
            pltpu.SemaphoreType.DMA((3, QKV_PARTS)),
            pltpu.SemaphoreType.DMA((2, 2, rows)),
            pltpu.SemaphoreType.DMA((2 * layers, 2, n_tp - 1)),
            pltpu.SemaphoreType.DMA((2 * layers, 2, n_tp - 1)),
        ],
        compiler_params=pltpu.CompilerParams(
            collective_id=0, has_side_effects=True, vmem_limit_bytes=VMEM_LIMIT),
        name='decode_step',
    )(positions, hidden, inv_freq, norm_scale, *caches, w_query, w_key, w_value, w_out, w_gate, w_up, w_down)
    hidden_out, *new_caches = pl.pallas_call(
        write_kernel,
        out_shape=tuple(jax.ShapeDtypeStruct(o.shape, o.dtype) for o in outs),
        in_specs=[hbm] * len(outs),
        out_specs=(hbm,) * len(outs),
        scratch_shapes=[pltpu.SemaphoreType.DMA((len(outs),))],
        compiler_params=pltpu.CompilerParams(vmem_limit_bytes=1024 * 1024),
        name='write_out',
    )(*outs)
    new_caches = [c.reshape(old.shape) for c, old in zip(new_caches, (k_local, v_local, k_global, v_global))]
    return (hidden_out, *new_caches)


def solution(mesh):
    row_spec = P('dp', None)
    cache_spec = P('dp', None, 'tp', None)
    col_split = P(None, None, 'tp')
    row_split = P(None, 'tp', None)
    in_specs = (row_spec, P('dp'), cache_spec, cache_spec, cache_spec, cache_spec, col_split, col_split, col_split, row_split, col_split, col_split, row_split, P())
    out_specs = (row_spec, cache_spec, cache_spec, cache_spec, cache_spec)
    return jax.shard_map(functools.partial(decode_step, mesh.shape['tp']), mesh=mesh, in_specs=in_specs, out_specs=out_specs, check_vma=False)
```

```python
import functools

import jax
import jax.numpy as jnp
import numpy as np
from jax import lax
from jax.experimental import pallas as pl
from jax.experimental.pallas import tpu as pltpu
from jax.sharding import PartitionSpec as P

SOFT_CAP = 50.0
NORM_EPS = 1e-6
ROPE_BASE = 10000.0

CHUNK = 256
SLOTS = 22
QKV_PARTS = 3
KV_STEP = 2048
GU_GROUP = 5
DN_GROUP = 3
QKV_CHUNKS, CACHE_CHUNKS = 4, 3
START_WINDOW, WINDOW, SUM_WINDOW = 10, 8, 20

VMEM_LIMIT = 52 * 1024 * 1024
WRITE_FLOPS = 20_000_000_000

F32 = jnp.float32
BF16 = jnp.bfloat16
MESH = pl.DeviceIdType.MESH


def rem(a, b):
    return a % b if isinstance(a, int) else lax.rem(a, b)


def far_first(n_tp):
    return sorted(range(1, n_tp), key=lambda step: -min(step, n_tp - step))


def split(count, group):
    return [min(group, count - i) for i in range(0, count, group)]


def rms_norm(values, gain_row):
    inv_rms = lax.rsqrt(jnp.mean(values * values, axis=-1, keepdims=True) + NORM_EPS)
    return (values * inv_rms * (1.0 + gain_row)).astype(BF16)


def step_kernel(n_tp, pos_in, hid_in, freq_in, norm_in, kl_in, vl_in, kg_in, vg_in, wq, wk, wv, wo, wg, wu, wd,
                hid_out, part_out, gain_out, kl, vl, kg, vg,
                pos_ref, hid_ref, freq_ref, norm_ref, ring, bq, bk, bv, x_ref, a_ref, o_ref, h_ref, acc, e_ref, part,
                small_sem, ring_sem, qkv_sem, cache_sem, send_sem, recv_sem):
    rows, width = hid_ref.shape
    head = kl.shape[2]
    half = head // 2
    ff = wg.shape[2]
    layers = wg.shape[0]
    n_wo = wo.shape[1] // CHUNK
    n_gu = width // CHUNK
    n_dn = ff // CHUNK
    dn_rest = ff - n_dn * CHUNK
    at_gu, at_dn = n_wo, n_wo + n_gu
    per_layer = n_wo + n_gu + n_dn + (1 if dn_rest else 0)
    me = lax.axis_index('tp')
    cut = pl.cdiv(width, 2 * CHUNK) * CHUNK
    pieces = ((0, cut), (cut, width - cut))

    def chunk_copies(kind, layer, k, slot):
        if kind == 'wo':
            return [pltpu.make_async_copy(wo.at[layer, pl.ds(k * CHUNK, CHUNK)], ring.at[slot], ring_sem.at[slot, 0])]
        if kind == 'gu':
            return [
                pltpu.make_async_copy(wg.at[layer, pl.ds(k * CHUNK, CHUNK)], ring.at[slot, :, pl.ds(0, ff)], ring_sem.at[slot, 0]),
                pltpu.make_async_copy(wu.at[layer, pl.ds(k * CHUNK, CHUNK)], ring.at[slot, :, pl.ds(ff, ff)], ring_sem.at[slot, 1]),
            ]
        if kind == 'dn':
            return [pltpu.make_async_copy(wd.at[layer, pl.ds(k * CHUNK, CHUNK)], ring.at[slot], ring_sem.at[slot, 0])]
        return [pltpu.make_async_copy(wd.at[layer, pl.ds(n_dn * CHUNK, dn_rest)], ring.at[slot, pl.ds(0, dn_rest)], ring_sem.at[slot, 0])]

    def chunk_of(c):
        layer, r = divmod(c, per_layer)
        if r < at_gu:
            return 'wo', layer, r
        if r < at_dn:
            return 'gu', layer, r - at_gu
        if r < at_dn + n_dn:
            return 'dn', layer, r - at_dn
        return 'rest', layer, 0

    queue = []
    for layer in range(layers):
        queue += [('qkv', layer), ('cache', layer)]
        queue += [('chunk', c) for c in range(layer * per_layer, (layer + 1) * per_layer)]
    state = {'next': 0, 'under_way': 0, 'free_chunks': SLOTS, 'free_qkv': 1}
    size_of = {'qkv': QKV_CHUNKS, 'cache': CACHE_CHUNKS, 'chunk': 1}

    def started(*item):
        assert queue.index(item) < state['next'], item

    def fill(limit, stop=None):
        while state['next'] < len(queue) and queue[state['next']] != stop:
            kind, index = queue[state['next']]
            if state['under_way'] and state['under_way'] + size_of[kind] > limit:
                return
            if kind == 'qkv':
                if index >= state['free_qkv']:
                    return
                for j in range(QKV_PARTS):
                    for copy in qkv_copies(index, j):
                        copy.start()
            elif kind == 'cache':
                for copy in cache_copies(index):
                    copy.start()
            else:
                if index >= state['free_chunks']:
                    return
                for copy in chunk_copies(*chunk_of(index), index % SLOTS):
                    copy.start()
            state['under_way'] += size_of[kind]
            state['next'] += 1

    def stream_dot(lhs_ref, layer, first, groups, phase):
        out = None
        row = 0
        c = layer * per_layer + first
        for g, group in enumerate(groups):
            members = range(c, c + group)
            for i in members:
                started('chunk', i)
                for copy in chunk_copies(*chunk_of(i), i % SLOTS):
                    copy.wait()
            state['under_way'] -= group
            fill(WINDOW)
            terms = []
            for i in members:
                n = dn_rest if chunk_of(i)[0] == 'rest' else CHUNK
                terms.append((lhs_ref[:, pl.ds(row, n)], i % SLOTS, n))
                row += n

            def product(columns):
                start, size = columns
                parts = [] if out is None else [out[:, start:start + size]]
                for lhs, slot, n in terms:
                    parts.append(jnp.dot(lhs, ring[slot, pl.ds(0, n), pl.ds(start, size)], preferred_element_type=F32))
                return functools.reduce(jnp.add, parts)

            state['free_chunks'] += group
            c += group
            if g < len(groups) - 1:
                out = product((0, width))
                continue
            if phase == 2 * layers - 1:
                part_out[...] = product((0, width)).astype(BF16)
                continue
            for p, columns in enumerate(pieces):
                part[phase, me, :, pl.ds(*columns)] = product(columns).astype(BF16)
                for copy in send_copies(phase, p):
                    copy.start()

    def stream_loop(lhs_ref, layer, first, kind, steps, group, in_loop):
        base = layer * per_layer + first
        acc[...] = jnp.zeros_like(acc)
        ahead = 0
        if state['next'] < len(queue) and queue[state['next']] == ('chunk', base + steps * group):
            ahead = min(in_loop, n_dn // steps)
        for _ in range(ahead * steps):
            assert chunk_of(queue[state['next']][1])[0] == 'dn' and queue[state['next']][1] < base + SLOTS
            state['next'] += 1
            state['under_way'] += 1

        started('chunk', base + steps * group - 1)

        def body(i, carry):
            members = [(i * group + j, rem(base + i * group + j, SLOTS)) for j in range(group)]
            for k, slot in members:
                for copy in chunk_copies(kind, layer, k, slot):
                    copy.wait()
            for j in range(ahead):
                for copy in chunk_copies('dn', layer, i * ahead + j, rem(base + steps * group + i * ahead + j, SLOTS)):
                    copy.start()
            out = acc[...]
            for k, slot in members:
                lhs = lhs_ref[:, pl.ds(pl.multiple_of(k * CHUNK, CHUNK), CHUNK)]
                out = out + jnp.dot(lhs, ring[slot], preferred_element_type=F32)
            acc[...] = out
            return carry

        lax.fori_loop(0, steps, body, 0)
        state['under_way'] -= steps * group
        state['free_chunks'] += steps * group
        fill(WINDOW)

    qkv_rows = width // QKV_PARTS

    def qkv_copies(layer, j):
        piece = pl.ds(j * qkv_rows, qkv_rows)
        return [pltpu.make_async_copy(src.at[layer, piece], dst.at[piece], qkv_sem.at[i, j])
                for i, (src, dst) in enumerate(((wq, bq), (wk, bk), (wv, bv)))]

    def cache_copies(layer):
        pairs = ((kl_in, kl), (vl_in, vl)) if layer == 0 else ((kg_in, kg), (vg_in, vg))
        return [pltpu.make_async_copy(src.at[b], dst.at[b], cache_sem.at[layer, i, b])
                for i, (src, dst) in enumerate(pairs) for b in range(rows)]

    def send_copies(phase, p):
        copies = []
        for step in far_first(n_tp):
            peer = lax.rem(me + step, n_tp)
            mine = part.at[phase, me, :, pl.ds(*pieces[p])]
            copies.append(pltpu.make_async_remote_copy(
                src_ref=mine, dst_ref=mine,
                send_sem=send_sem.at[phase, p, step - 1], recv_sem=recv_sem.at[phase, p, step - 1],
                device_id={'tp': peer}, device_id_type=MESH))
        return copies

    def collect(phase, limit, stop=None, meanwhile=None):
        fill(limit, stop)
        if meanwhile is not None:
            meanwhile()
        sums = []
        for p, columns in enumerate(pieces):
            for copy in send_copies(phase, p):
                copy.wait_recv()
            total = part[phase, 0, :, pl.ds(*columns)].astype(F32)
            for j in range(1, n_tp):
                total = total + part[phase, j, :, pl.ds(*columns)].astype(F32)
            sums.append(total)
        return jnp.concatenate(sums, axis=-1)

    def gain(layer, i):
        return norm_ref[layer, pl.ds(i, 1), :]

    def add_normed(layer, i, branch_sum):
        x = (x_ref[...] + rms_norm(branch_sum, gain(layer, i)).astype(F32)).astype(BF16)
        x_ref[...] = x.astype(F32)
        return x

    def rotate(values, trig):
        first, second = values[:, :half], values[:, half:]
        cos_part, sin_part = trig
        return jnp.concatenate([first * cos_part - second * sin_part, second * cos_part + first * sin_part], axis=-1)

    def store_row(cache, b, slot, new_row):
        n = cache.shape[1]
        step = min(n, KV_STEP)

        def body(i, carry):
            piece = pl.ds(pl.multiple_of(i * step, step), step)
            ids = lax.broadcasted_iota(jnp.int32, (step, head), 0) + i * step
            cache[b, piece] = jnp.where(ids == slot, jnp.broadcast_to(new_row, (step, head)), cache[b, piece])
            return carry

        lax.fori_loop(0, n // step, body, 0)

    def attention(layer, kc, vc, trig):
        n = kc.shape[1]
        a_ref[...] = rms_norm(x_ref[...], gain(layer, 0))
        hq = bq.shape[1]

        started('qkv', layer)

        def qkv_body(j, carry):
            q, k, v = carry
            for copy in qkv_copies(layer, j):
                copy.wait()
            piece = pl.ds(pl.multiple_of(j * qkv_rows, qkv_rows), qkv_rows)
            lhs = a_ref[:, piece]
            q = q + jnp.dot(lhs, bq[piece], preferred_element_type=F32)
            k = k + jnp.dot(lhs, bk[piece], preferred_element_type=F32)
            v = v + jnp.dot(lhs, bv[piece], preferred_element_type=F32)
            return q, k, v

        q, k, v = lax.fori_loop(0, QKV_PARTS, qkv_body, (
            jnp.zeros((rows, hq), F32), jnp.zeros((rows, head), F32), jnp.zeros((rows, head), F32)))
        state['under_way'] -= QKV_CHUNKS
        state['free_qkv'] += 1
        fill(WINDOW)
        group = hq // head
        queries = jnp.concatenate([rotate(q[:, g * head:(g + 1) * head], trig) for g in range(group)], axis=0).astype(BF16)
        k_new = rotate(k, trig).astype(BF16)
        v_new = v.astype(BF16)
        started('cache', layer)
        for copy in cache_copies(layer):
            copy.wait()
        state['under_way'] -= CACHE_CHUNKS
        fill(WINDOW)
        q_rows = group * rows
        row_seq = lax.rem(lax.broadcasted_iota(jnp.int32, (q_rows, 1), 0), rows)
        last, slot = jnp.zeros((q_rows, 1), jnp.int32), jnp.zeros((q_rows, 1), jnp.int32)
        for b in range(rows):
            last = jnp.where(row_seq == b, pos_ref[b], last)
            slot = jnp.where(row_seq == b, lax.rem(pos_ref[b], n), slot)

        def pick(per_seq):
            out = per_seq[0]
            for b in range(1, rows):
                out = jnp.where(row_seq == b, per_seq[b], out)
            return out

        step = min(n, KV_STEP)
        contract_last = (((1,), (1,)), ((), ()))

        def soft_exp(s):
            return jnp.exp(SOFT_CAP * jnp.tanh(s * (head ** -0.5 / SOFT_CAP)))

        per_row = [jnp.concatenate([new.astype(F32)] * group, axis=0) for new in (k_new, v_new)]
        e_new = soft_exp(jnp.sum(queries.astype(F32) * per_row[0], axis=-1, keepdims=True))
        total = e_new
        def score_body(i, total):
            piece = pl.ds(pl.multiple_of(i * step, step), step)
            s = pick([lax.dot_general(queries, kc[b, piece], contract_last, preferred_element_type=F32) for b in range(rows)])
            ids = lax.broadcasted_iota(jnp.int32, (q_rows, step), 1) + i * step
            e = jnp.where((ids <= last) & (ids != slot), soft_exp(s), 0.0)
            e_ref[:, piece] = e
            return total + jnp.sum(e, axis=-1, keepdims=True)

        total = lax.fori_loop(0, n // step, score_body, total)

        def value_body(i, out):
            piece = pl.ds(pl.multiple_of(i * step, step), step)
            probs = (e_ref[:, piece] * inv_total).astype(BF16)
            return out + pick([jnp.dot(probs, vc[b, piece], preferred_element_type=F32) for b in range(rows)])

        inv_total = 1.0 / total
        out = (e_new * inv_total).astype(BF16).astype(F32) * per_row[1]
        out = lax.fori_loop(0, n // step, value_body, out)
        mixed = out.astype(BF16)
        for g in range(group):
            o_ref[:, pl.ds(g * head, head)] = mixed[g * rows:(g + 1) * rows]

        def store_new():
            for b in range(rows):
                store_row(kc, b, lax.rem(pos_ref[b], n), k_new[b:b + 1])
                store_row(vc, b, lax.rem(pos_ref[b], n), v_new[b:b + 1])

        return store_new

    small = [pltpu.make_async_copy(src, dst, small_sem.at[i]) for i, (src, dst) in enumerate(
        ((hid_in, hid_ref), (norm_in, norm_ref), (pos_in, pos_ref), (freq_in, freq_ref)))]
    for copy in small:
        copy.start()
    fill(START_WINDOW)

    barrier = pltpu.get_barrier_semaphore()
    for step in range(1, n_tp):
        pl.semaphore_signal(barrier, inc=1, device_id={'tp': lax.rem(me + step, n_tp)}, device_id_type=MESH)

    for copy in small:
        copy.wait()
    x_ref[...] = hid_ref[...].astype(F32)
    row_ids = lax.broadcasted_iota(jnp.int32, (rows, half), 0)
    pos_rows = jnp.zeros((rows, half), F32)
    for b in range(rows):
        pos_rows = jnp.where(row_ids == b, pos_ref[b].astype(F32), pos_rows)
    angles = pos_rows * freq_ref[...]
    trig = jnp.cos(angles), jnp.sin(angles)
    for layer in range(layers):
        kc, vc = (kl, vl) if layer == 0 else (kg, vg)
        store_new = attention(layer, kc, vc, trig)
        if layer == 0:
            pl.semaphore_wait(barrier, n_tp - 1)
        stream_dot(o_ref, layer, 0, (n_wo,), 2 * layer)
        x = add_normed(layer, 1, collect(2 * layer, len(queue) * QKV_CHUNKS, ('chunk', at_dn), store_new))
        a_ref[...] = rms_norm(x.astype(F32), gain(layer, 2))
        stream_loop(a_ref, layer, at_gu, 'gu', n_gu // GU_GROUP, GU_GROUP, 2)
        gate_up = acc[...]
        h_ref[...] = (jax.nn.gelu(gate_up[:, :ff], approximate=True) * gate_up[:, ff:]).astype(BF16)
        stream_dot(h_ref, layer, at_dn, split(per_layer - at_dn, DN_GROUP), 2 * layer + 1)
        if layer < layers - 1:
            x = add_normed(layer, 3, collect(2 * layer + 1, SUM_WINDOW))
    hid_out[...] = x
    gain_out[...] = gain(layers - 1, 3)
    for phase in range(2 * layers - 1):
        for p in range(len(pieces)):
            for copy in send_copies(phase, p):
                copy.wait_send()


def write_kernel(*refs):
    n = len(refs) // 2
    copies = [pltpu.make_async_copy(refs[i], refs[n + i], refs[-1].at[i]) for i in range(n)]
    for copy in copies:
        copy.start()
    for copy in copies:
        copy.wait()


def finish_kernel(n_tp, x_ref, gain_ref, *refs):
    *parts, out_ref, part = refs
    me = lax.axis_index('tp')
    for step in range(n_tp):
        part[lax.rem(me + n_tp - step, n_tp)] = parts[step][...]
    total = part[0].astype(F32)
    for j in range(1, n_tp):
        total = total + part[j].astype(F32)
    out_ref[...] = (x_ref[...].astype(F32) + rms_norm(total, gain_ref[...]).astype(F32)).astype(BF16)


def decode_step(n_tp, hidden, positions, k_local, v_local, k_global, v_global, w_query, w_key, w_value, w_out, w_gate, w_up, w_down, norm_scale):
    rows, width = hidden.shape
    caches = [c.reshape(c.shape[0], c.shape[1], c.shape[3]) for c in (k_local, v_local, k_global, v_global)]
    head = caches[0].shape[2]
    half = head // 2
    inv_freq = jnp.asarray(ROPE_BASE ** (-2.0 * np.arange(half) / head), F32)[None, :]
    hq, ff, layers = w_query.shape[2], w_gate.shape[2], w_gate.shape[0]
    n_ctx = max(c.shape[1] for c in caches)
    vmem = pl.BlockSpec(memory_space=pltpu.VMEM)
    hbm = pl.BlockSpec(memory_space=pl.ANY)
    outs = pl.pallas_call(
        functools.partial(step_kernel, n_tp),
        out_shape=tuple(pltpu.VMEM(a.shape, BF16) for a in (hidden, hidden)) + (pltpu.VMEM((1, width), F32),) + tuple(pltpu.VMEM(a.shape, BF16) for a in caches),
        in_specs=[hbm] * 15,
        out_specs=(vmem,) * 7,
        scratch_shapes=[
            pltpu.SMEM((rows,), jnp.int32),
            pltpu.VMEM((rows, width), BF16),
            pltpu.VMEM((1, half), F32),
            pltpu.VMEM(norm_scale.shape, F32),
            pltpu.VMEM((SLOTS, CHUNK, width), BF16),
            pltpu.VMEM((width, hq), BF16),
            pltpu.VMEM((width, head), BF16),
            pltpu.VMEM((width, head), BF16),
            pltpu.VMEM((rows, width), F32),
            pltpu.VMEM((rows, width), BF16),
            pltpu.VMEM((rows, hq), BF16),
            pltpu.VMEM((rows, ff), BF16),
            pltpu.VMEM((rows, 2 * ff), F32),
            pltpu.VMEM((hq // head * rows, n_ctx), F32),
            pltpu.VMEM((2 * layers, n_tp, rows, width), BF16),
            pltpu.SemaphoreType.DMA((4,)),
            pltpu.SemaphoreType.DMA((SLOTS, 2)),
            pltpu.SemaphoreType.DMA((3, QKV_PARTS)),
            pltpu.SemaphoreType.DMA((2, 2, rows)),
            pltpu.SemaphoreType.DMA((2 * layers, 2, n_tp - 1)),
            pltpu.SemaphoreType.DMA((2 * layers, 2, n_tp - 1)),
        ],
        compiler_params=pltpu.CompilerParams(
            collective_id=0, has_side_effects=True, vmem_limit_bytes=VMEM_LIMIT),
        name='decode_step',
    )(positions, hidden, inv_freq, norm_scale, *caches, w_query, w_key, w_value, w_out, w_gate, w_up, w_down)
    x, partial, gain_row, *new_caches = outs
    received = [lax.ppermute(partial, 'tp', [(i, (i + step) % n_tp) for i in range(n_tp)]) for step in range(1, n_tp)]
    new_caches = pl.pallas_call(
        write_kernel,
        out_shape=tuple(jax.ShapeDtypeStruct(o.shape, o.dtype) for o in new_caches),
        in_specs=[hbm] * len(new_caches),
        out_specs=(hbm,) * len(new_caches),
        scratch_shapes=[pltpu.SemaphoreType.DMA((len(new_caches),))],
        compiler_params=pltpu.CompilerParams(vmem_limit_bytes=1024 * 1024),
        cost_estimate=pl.CostEstimate(flops=WRITE_FLOPS, bytes_accessed=sum(2 * o.size for o in new_caches), transcendentals=0),
        name='write_out',
    )(*new_caches)
    hidden_out = pl.pallas_call(
        functools.partial(finish_kernel, n_tp),
        out_shape=jax.ShapeDtypeStruct(hidden.shape, BF16),
        in_specs=[vmem] * (2 + n_tp),
        out_specs=vmem,
        scratch_shapes=[pltpu.VMEM((n_tp, rows, width), BF16)],
        compiler_params=pltpu.CompilerParams(vmem_limit_bytes=2 * 1024 * 1024),
        name='finish',
    )(x, gain_row, partial, *received)
    new_caches = [c.reshape(old.shape) for c, old in zip(new_caches, (k_local, v_local, k_global, v_global))]
    return (hidden_out, *new_caches)


def solution(mesh):
    row_spec = P('dp', None)
    cache_spec = P('dp', None, 'tp', None)
    col_split = P(None, None, 'tp')
    row_split = P(None, 'tp', None)
    in_specs = (row_spec, P('dp'), cache_spec, cache_spec, cache_spec, cache_spec, col_split, col_split, col_split, row_split, col_split, col_split, row_split, P())
    out_specs = (row_spec, cache_spec, cache_spec, cache_spec, cache_spec)
    return jax.shard_map(functools.partial(decode_step, mesh.shape['tp']), mesh=mesh, in_specs=in_specs, out_specs=out_specs, check_vma=False)
```

```python
import functools

import jax
import jax.numpy as jnp
import numpy as np
from jax import lax
from jax.experimental import pallas as pl
from jax.experimental.pallas import tpu as pltpu
from jax.sharding import PartitionSpec as P

SOFT_CAP = 50.0
NORM_EPS = 1e-6
ROPE_BASE = 10000.0

CHUNK = 256
SLOTS = 22
QKV_PARTS = 3
KV_STEP = 2048
GU_GROUP = 5
DN_GROUP = 3
QKV_CHUNKS, CACHE_CHUNKS = 4, 3
START_WINDOW, WINDOW, SUM_WINDOW = 10, 8, 20

VMEM_LIMIT = 52 * 1024 * 1024

F32 = jnp.float32
BF16 = jnp.bfloat16
MESH = pl.DeviceIdType.MESH


def rem(a, b):
    return a % b if isinstance(a, int) else lax.rem(a, b)


def far_first(n_tp):
    return sorted(range(1, n_tp), key=lambda step: -min(step, n_tp - step))


def split(count, group):
    return [min(group, count - i) for i in range(0, count, group)]


def rms_norm(values, gain_row):
    inv_rms = lax.rsqrt(jnp.mean(values * values, axis=-1, keepdims=True) + NORM_EPS)
    return (values * inv_rms * (1.0 + gain_row)).astype(BF16)


def step_kernel(n_tp, pos_in, hid_in, freq_in, norm_in, kl_in, vl_in, kg_in, vg_in, wq, wk, wv, wo, wg, wu, wd,
                hid_out, kl, vl, kg, vg,
                pos_ref, hid_ref, freq_ref, norm_ref, ring, bq, bk, bv, x_ref, a_ref, o_ref, h_ref, acc, e_ref, part,
                small_sem, ring_sem, qkv_sem, cache_sem, send_sem, recv_sem):
    rows, width = hid_ref.shape
    head = kl.shape[2]
    half = head // 2
    ff = wg.shape[2]
    layers = wg.shape[0]
    n_wo = wo.shape[1] // CHUNK
    n_gu = width // CHUNK
    n_dn = ff // CHUNK
    dn_rest = ff - n_dn * CHUNK
    at_gu, at_dn = n_wo, n_wo + n_gu
    per_layer = n_wo + n_gu + n_dn + (1 if dn_rest else 0)
    me = lax.axis_index('tp')

    def chunk_copies(kind, layer, k, slot):
        if kind == 'wo':
            return [pltpu.make_async_copy(wo.at[layer, pl.ds(k * CHUNK, CHUNK)], ring.at[slot], ring_sem.at[slot])]
        if kind == 'gu':
            return [
                pltpu.make_async_copy(wg.at[layer, pl.ds(k * CHUNK, CHUNK)], ring.at[slot, :, pl.ds(0, ff)], ring_sem.at[slot]),
                pltpu.make_async_copy(wu.at[layer, pl.ds(k * CHUNK, CHUNK)], ring.at[slot, :, pl.ds(ff, ff)], ring_sem.at[slot]),
            ]
        if kind == 'dn':
            return [pltpu.make_async_copy(wd.at[layer, pl.ds(k * CHUNK, CHUNK)], ring.at[slot], ring_sem.at[slot])]
        return [pltpu.make_async_copy(wd.at[layer, pl.ds(n_dn * CHUNK, dn_rest)], ring.at[slot, pl.ds(0, dn_rest)], ring_sem.at[slot])]

    def wait_chunk(kind, slot):
        place = ring.at[slot, pl.ds(0, dn_rest)] if kind == 'rest' else ring.at[slot]
        pltpu.make_async_copy(place, place, ring_sem.at[slot]).wait()

    def chunk_of(c):
        layer, r = divmod(c, per_layer)
        if r < at_gu:
            return 'wo', layer, r
        if r < at_dn:
            return 'gu', layer, r - at_gu
        if r < at_dn + n_dn:
            return 'dn', layer, r - at_dn
        return 'rest', layer, 0

    queue = []
    for layer in range(layers):
        queue += [('qkv', layer), ('cache', layer)]
        queue += [('chunk', c) for c in range(layer * per_layer, (layer + 1) * per_layer)]
    state = {'next': 0, 'under_way': 0, 'free_chunks': SLOTS, 'free_qkv': 1}
    size_of = {'qkv': QKV_CHUNKS, 'cache': CACHE_CHUNKS, 'chunk': 1}

    def started(*item):
        assert queue.index(item) < state['next'], item

    def fill(limit, stop=None):
        while state['next'] < len(queue) and queue[state['next']] != stop:
            kind, index = queue[state['next']]
            if state['under_way'] and state['under_way'] + size_of[kind] > limit:
                return
            if kind == 'qkv':
                if index >= state['free_qkv']:
                    return
                for j in range(QKV_PARTS):
                    for copy in qkv_copies(index, j):
                        copy.start()
            elif kind == 'cache':
                for copy in cache_copies(index):
                    copy.start()
            else:
                if index >= state['free_chunks']:
                    return
                for copy in chunk_copies(*chunk_of(index), index % SLOTS):
                    copy.start()
            state['under_way'] += size_of[kind]
            state['next'] += 1

    def stream_dot(lhs_ref, layer, first, groups):
        out = jnp.zeros(acc.shape, F32)
        row = 0
        c = layer * per_layer + first
        for group in groups:
            members = range(c, c + group)
            for i in members:
                started('chunk', i)
                wait_chunk(chunk_of(i)[0], i % SLOTS)
            state['under_way'] -= group
            fill(WINDOW)
            for i in members:
                n = dn_rest if chunk_of(i)[0] == 'rest' else CHUNK
                out = out + jnp.dot(lhs_ref[:, pl.ds(row, n)], ring[i % SLOTS, pl.ds(0, n)], preferred_element_type=F32)
                row += n
            state['free_chunks'] += group
            c += group
        acc[...] = out
        fill(WINDOW)

    def stream_loop(lhs_ref, layer, first, kind, steps, group, in_loop):
        base = layer * per_layer + first
        acc[...] = jnp.zeros_like(acc)
        ahead = 0
        if state['next'] < len(queue) and queue[state['next']] == ('chunk', base + steps * group):
            ahead = min(in_loop, n_dn // steps)
        for _ in range(ahead * steps):
            assert chunk_of(queue[state['next']][1])[0] == 'dn' and queue[state['next']][1] < base + SLOTS
            state['next'] += 1
            state['under_way'] += 1

        started('chunk', base + steps * group - 1)

        def body(i, carry):
            members = [(i * group + j, rem(base + i * group + j, SLOTS)) for j in range(group)]
            for k, slot in members:
                wait_chunk(kind, slot)
            for j in range(ahead):
                for copy in chunk_copies('dn', layer, i * ahead + j, rem(base + steps * group + i * ahead + j, SLOTS)):
                    copy.start()
            out = acc[...]
            for k, slot in members:
                lhs = lhs_ref[:, pl.ds(pl.multiple_of(k * CHUNK, CHUNK), CHUNK)]
                out = out + jnp.dot(lhs, ring[slot], preferred_element_type=F32)
            acc[...] = out
            return carry

        lax.fori_loop(0, steps, body, 0)
        state['under_way'] -= steps * group
        state['free_chunks'] += steps * group
        fill(WINDOW)

    qkv_rows = width // QKV_PARTS

    def qkv_copies(layer, j):
        piece = pl.ds(j * qkv_rows, qkv_rows)
        return [pltpu.make_async_copy(src.at[layer, piece], dst.at[piece], qkv_sem.at[i, j])
                for i, (src, dst) in enumerate(((wq, bq), (wk, bk), (wv, bv)))]

    def cache_copies(layer):
        pairs = ((kl_in, kl), (vl_in, vl)) if layer == 0 else ((kg_in, kg), (vg_in, vg))
        return [pltpu.make_async_copy(src.at[b], dst.at[b], cache_sem.at[layer, i, b])
                for i, (src, dst) in enumerate(pairs) for b in range(rows)]

    def send_copies(phase):
        copies = []
        for step in far_first(n_tp):
            peer = lax.rem(me + step, n_tp)
            copies.append(pltpu.make_async_remote_copy(
                src_ref=part.at[phase, me], dst_ref=part.at[phase, me],
                send_sem=send_sem.at[phase], recv_sem=recv_sem.at[phase],
                device_id={'tp': peer}, device_id_type=MESH))
        return copies

    def all_copies(phase):
        blocks = part.at[phase, pl.ds(0, n_tp - 1)]
        return pltpu.make_async_remote_copy(
            src_ref=blocks, dst_ref=blocks, send_sem=send_sem.at[phase], recv_sem=recv_sem.at[phase],
            device_id={'tp': me}, device_id_type=MESH)

    def exchange(phase, limit, stop=None, meanwhile=None):
        part[phase, me] = acc[...].astype(BF16)
        copies = send_copies(phase)
        for copy in copies:
            copy.start()
        fill(limit, stop)
        if meanwhile is not None:
            meanwhile()
        all_copies(phase).wait_recv()
        total = part[phase, 0].astype(F32)
        for j in range(1, n_tp):
            total = total + part[phase, j].astype(F32)
        return total

    def gain(layer, i):
        return norm_ref[layer, pl.ds(i, 1), :]

    def add_normed(layer, i, branch_sum):
        x = (x_ref[...] + rms_norm(branch_sum, gain(layer, i)).astype(F32)).astype(BF16)
        x_ref[...] = x.astype(F32)
        return x

    def rotate(values, trig):
        first, second = values[:, :half], values[:, half:]
        cos_part, sin_part = trig
        return jnp.concatenate([first * cos_part - second * sin_part, second * cos_part + first * sin_part], axis=-1)

    def store_row(cache, b, slot, new_row):
        n = cache.shape[1]
        step = min(n, KV_STEP)

        def body(i, carry):
            piece = pl.ds(pl.multiple_of(i * step, step), step)
            ids = lax.broadcasted_iota(jnp.int32, (step, head), 0) + i * step
            cache[b, piece] = jnp.where(ids == slot, jnp.broadcast_to(new_row, (step, head)), cache[b, piece])
            return carry

        lax.fori_loop(0, n // step, body, 0)

    def attention(layer, kc, vc, trig):
        n = kc.shape[1]
        a_ref[...] = rms_norm(x_ref[...], gain(layer, 0))
        hq = bq.shape[1]

        started('qkv', layer)

        def qkv_body(j, carry):
            q, k, v = carry
            for copy in qkv_copies(layer, j):
                copy.wait()
            piece = pl.ds(pl.multiple_of(j * qkv_rows, qkv_rows), qkv_rows)
            lhs = a_ref[:, piece]
            q = q + jnp.dot(lhs, bq[piece], preferred_element_type=F32)
            k = k + jnp.dot(lhs, bk[piece], preferred_element_type=F32)
            v = v + jnp.dot(lhs, bv[piece], preferred_element_type=F32)
            return q, k, v

        q, k, v = lax.fori_loop(0, QKV_PARTS, qkv_body, (
            jnp.zeros((rows, hq), F32), jnp.zeros((rows, head), F32), jnp.zeros((rows, head), F32)))
        state['under_way'] -= QKV_CHUNKS
        state['free_qkv'] += 1
        fill(WINDOW)
        group = hq // head
        queries = jnp.concatenate([rotate(q[:, g * head:(g + 1) * head], trig) for g in range(group)], axis=0).astype(BF16)
        k_new = rotate(k, trig).astype(BF16)
        v_new = v.astype(BF16)
        started('cache', layer)
        for copy in cache_copies(layer):
            copy.wait()
        state['under_way'] -= CACHE_CHUNKS
        fill(WINDOW)
        q_rows = group * rows
        row_seq = lax.rem(lax.broadcasted_iota(jnp.int32, (q_rows, 1), 0), rows)
        last, slot = jnp.zeros((q_rows, 1), jnp.int32), jnp.zeros((q_rows, 1), jnp.int32)
        for b in range(rows):
            last = jnp.where(row_seq == b, pos_ref[b], last)
            slot = jnp.where(row_seq == b, lax.rem(pos_ref[b], n), slot)

        def pick(per_seq):
            out = per_seq[0]
            for b in range(1, rows):
                out = jnp.where(row_seq == b, per_seq[b], out)
            return out

        step = min(n, KV_STEP)
        contract_last = (((1,), (1,)), ((), ()))

        def soft_exp(s):
            return jnp.exp(SOFT_CAP * jnp.tanh(s * (head ** -0.5 / SOFT_CAP)))

        per_row = [jnp.concatenate([new.astype(F32)] * group, axis=0) for new in (k_new, v_new)]
        e_new = soft_exp(jnp.sum(queries.astype(F32) * per_row[0], axis=-1, keepdims=True))
        total = e_new
        def score_body(i, total):
            piece = pl.ds(pl.multiple_of(i * step, step), step)
            s = pick([lax.dot_general(queries, kc[b, piece], contract_last, preferred_element_type=F32) for b in range(rows)])
            ids = lax.broadcasted_iota(jnp.int32, (q_rows, step), 1) + i * step
            e = jnp.where((ids <= last) & (ids != slot), soft_exp(s), 0.0)
            e_ref[:, piece] = e
            return total + jnp.sum(e, axis=-1, keepdims=True)

        total = lax.fori_loop(0, n // step, score_body, total)

        def value_body(i, out):
            piece = pl.ds(pl.multiple_of(i * step, step), step)
            probs = (e_ref[:, piece] * inv_total).astype(BF16)
            return out + pick([jnp.dot(probs, vc[b, piece], preferred_element_type=F32) for b in range(rows)])

        inv_total = 1.0 / total
        out = (e_new * inv_total).astype(BF16).astype(F32) * per_row[1]
        out = lax.fori_loop(0, n // step, value_body, out)
        mixed = out.astype(BF16)
        for g in range(group):
            o_ref[:, pl.ds(g * head, head)] = mixed[g * rows:(g + 1) * rows]

        def store_new():
            for b in range(rows):
                store_row(kc, b, lax.rem(pos_ref[b], n), k_new[b:b + 1])
                store_row(vc, b, lax.rem(pos_ref[b], n), v_new[b:b + 1])

        return store_new

    small = [pltpu.make_async_copy(src, dst, small_sem.at[i]) for i, (src, dst) in enumerate(
        ((hid_in, hid_ref), (norm_in, norm_ref), (pos_in, pos_ref), (freq_in, freq_ref)))]
    for copy in small:
        copy.start()
    fill(START_WINDOW)

    barrier = pltpu.get_barrier_semaphore()
    for step in range(1, n_tp):
        pl.semaphore_signal(barrier, inc=1, device_id={'tp': lax.rem(me + step, n_tp)}, device_id_type=MESH)

    for copy in small:
        copy.wait()
    x_ref[...] = hid_ref[...].astype(F32)
    row_ids = lax.broadcasted_iota(jnp.int32, (rows, half), 0)
    pos_rows = jnp.zeros((rows, half), F32)
    for b in range(rows):
        pos_rows = jnp.where(row_ids == b, pos_ref[b].astype(F32), pos_rows)
    angles = pos_rows * freq_ref[...]
    trig = jnp.cos(angles), jnp.sin(angles)
    for layer in range(layers):
        kc, vc = (kl, vl) if layer == 0 else (kg, vg)
        store_new = attention(layer, kc, vc, trig)
        stream_dot(o_ref, layer, 0, (n_wo,))
        if layer == 0:
            pl.semaphore_wait(barrier, n_tp - 1)
        x = add_normed(layer, 1, exchange(2 * layer, len(queue) * QKV_CHUNKS, ('chunk', at_dn), store_new))
        a_ref[...] = rms_norm(x.astype(F32), gain(layer, 2))
        stream_loop(a_ref, layer, at_gu, 'gu', n_gu // GU_GROUP, GU_GROUP, 2)
        gate_up = acc[...]
        h_ref[...] = (jax.nn.gelu(gate_up[:, :ff], approximate=True) * gate_up[:, ff:]).astype(BF16)
        stream_dot(h_ref, layer, at_dn, split(per_layer - at_dn, DN_GROUP))
        x = add_normed(layer, 3, exchange(2 * layer + 1, SUM_WINDOW))
    hid_out[...] = x
    for phase in range(2 * layers):
        all_copies(phase).wait_send()


def write_kernel(*refs):
    n = len(refs) // 2
    copies = [pltpu.make_async_copy(refs[i], refs[n + i], refs[-1].at[i]) for i in range(n)]
    for copy in copies:
        copy.start()
    for copy in copies:
        copy.wait()


def decode_step(n_tp, hidden, positions, k_local, v_local, k_global, v_global, w_query, w_key, w_value, w_out, w_gate, w_up, w_down, norm_scale):
    rows, width = hidden.shape
    caches = [c.reshape(c.shape[0], c.shape[1], c.shape[3]) for c in (k_local, v_local, k_global, v_global)]
    head = caches[0].shape[2]
    half = head // 2
    inv_freq = jnp.asarray(ROPE_BASE ** (-2.0 * np.arange(half) / head), F32)[None, :]
    hq, ff, layers = w_query.shape[2], w_gate.shape[2], w_gate.shape[0]
    n_ctx = max(c.shape[1] for c in caches)
    vmem = pl.BlockSpec(memory_space=pltpu.VMEM)
    hbm = pl.BlockSpec(memory_space=pl.ANY)
    outs = pl.pallas_call(
        functools.partial(step_kernel, n_tp),
        out_shape=tuple(pltpu.VMEM(a.shape, BF16) for a in (hidden, *caches)),
        in_specs=[hbm] * 15,
        out_specs=(vmem,) * 5,
        scratch_shapes=[
            pltpu.SMEM((rows,), jnp.int32),
            pltpu.VMEM((rows, width), BF16),
            pltpu.VMEM((1, half), F32),
            pltpu.VMEM(norm_scale.shape, F32),
            pltpu.VMEM((SLOTS, CHUNK, width), BF16),
            pltpu.VMEM((width, hq), BF16),
            pltpu.VMEM((width, head), BF16),
            pltpu.VMEM((width, head), BF16),
            pltpu.VMEM((rows, width), F32),
            pltpu.VMEM((rows, width), BF16),
            pltpu.VMEM((rows, hq), BF16),
            pltpu.VMEM((rows, ff), BF16),
            pltpu.VMEM((rows, 2 * ff), F32),
            pltpu.VMEM((hq // head * rows, n_ctx), F32),
            pltpu.VMEM((2 * layers, n_tp, rows, width), BF16),
            pltpu.SemaphoreType.DMA((4,)),
            pltpu.SemaphoreType.DMA((SLOTS,)),
            pltpu.SemaphoreType.DMA((3, QKV_PARTS)),
            pltpu.SemaphoreType.DMA((2, 2, rows)),
            pltpu.SemaphoreType.DMA((2 * layers,)),
            pltpu.SemaphoreType.DMA((2 * layers,)),
        ],
        compiler_params=pltpu.CompilerParams(
            collective_id=0, has_side_effects=True, vmem_limit_bytes=VMEM_LIMIT),
        name='decode_step',
    )(positions, hidden, inv_freq, norm_scale, *caches, w_query, w_key, w_value, w_out, w_gate, w_up, w_down)
    hidden_out, *new_caches = pl.pallas_call(
        write_kernel,
        out_shape=tuple(jax.ShapeDtypeStruct(o.shape, o.dtype) for o in outs),
        in_specs=[hbm] * len(outs),
        out_specs=(hbm,) * len(outs),
        scratch_shapes=[pltpu.SemaphoreType.DMA((len(outs),))],
        compiler_params=pltpu.CompilerParams(vmem_limit_bytes=1024 * 1024),
        name='write_out',
    )(*outs)
    new_caches = [c.reshape(old.shape) for c, old in zip(new_caches, (k_local, v_local, k_global, v_global))]
    return (hidden_out, *new_caches)


def solution(mesh):
    row_spec = P('dp', None)
    cache_spec = P('dp', None, 'tp', None)
    col_split = P(None, None, 'tp')
    row_split = P(None, 'tp', None)
    in_specs = (row_spec, P('dp'), cache_spec, cache_spec, cache_spec, cache_spec, col_split, col_split, col_split, row_split, col_split, col_split, row_split, P())
    out_specs = (row_spec, cache_spec, cache_spec, cache_spec, cache_spec)
    return jax.shard_map(functools.partial(decode_step, mesh.shape['tp']), mesh=mesh, in_specs=in_specs, out_specs=out_specs, check_vma=False)
```

```python
import functools

import jax
import jax.numpy as jnp
import numpy as np
from jax import lax
from jax.experimental import pallas as pl
from jax.experimental.pallas import tpu as pltpu
from jax.sharding import PartitionSpec as P

SOFT_CAP = 50.0
NORM_EPS = 1e-6
ROPE_BASE = 10000.0

CHUNK = 256
SLOTS = 22
QKV_PARTS = 3
KV_STEP = 2048
GU_GROUP = 5
DN_GROUP = 3
LATE_DN_GROUP = 3
QKV_CHUNKS, CACHE_CHUNKS = 4, 3
START_WINDOW, WINDOW, SUM_WINDOW = 10, 8, 32

VMEM_LIMIT = 52 * 1024 * 1024

F32 = jnp.float32
BF16 = jnp.bfloat16
MESH = pl.DeviceIdType.MESH


def rem(a, b):
    return a % b if isinstance(a, int) else lax.rem(a, b)


def far_first(n_tp):
    return sorted(range(1, n_tp), key=lambda step: -min(step, n_tp - step))


def split(count, group):
    return [min(group, count - i) for i in range(0, count, group)]


def rms_norm(values, gain_row):
    inv_rms = lax.rsqrt(jnp.mean(values * values, axis=-1, keepdims=True) + NORM_EPS)
    return (values * inv_rms * (1.0 + gain_row)).astype(BF16)


def step_kernel(n_tp, pos_in, hid_in, freq_in, norm_in, kl_in, vl_in, kg_in, vg_in, wq, wk, wv, wo, wg, wu, wd,
                hid_out, kl, vl, kg, vg,
                pos_ref, hid_ref, freq_ref, norm_ref, ring, bq, bk, bv, x_ref, a_ref, o_ref, h_ref, acc, e_ref, part,
                small_sem, ring_sem, qkv_sem, cache_sem, send_sem, recv_sem):
    rows, width = hid_ref.shape
    head = kl.shape[2]
    half = head // 2
    ff = wg.shape[2]
    layers = wg.shape[0]
    n_wo = wo.shape[1] // CHUNK
    n_gu = width // CHUNK
    n_dn = ff // CHUNK
    dn_rest = ff - n_dn * CHUNK
    at_gu, at_dn = n_wo, n_wo + n_gu
    per_layer = n_wo + n_gu + n_dn + (1 if dn_rest else 0)
    me = lax.axis_index('tp')

    def chunk_copies(kind, layer, k, slot):
        if kind == 'wo':
            return [pltpu.make_async_copy(wo.at[layer, pl.ds(k * CHUNK, CHUNK)], ring.at[slot], ring_sem.at[slot])]
        if kind == 'gu':
            return [
                pltpu.make_async_copy(wg.at[layer, pl.ds(k * CHUNK, CHUNK)], ring.at[slot, :, pl.ds(0, ff)], ring_sem.at[slot]),
                pltpu.make_async_copy(wu.at[layer, pl.ds(k * CHUNK, CHUNK)], ring.at[slot, :, pl.ds(ff, ff)], ring_sem.at[slot]),
            ]
        if kind == 'dn':
            return [pltpu.make_async_copy(wd.at[layer, pl.ds(k * CHUNK, CHUNK)], ring.at[slot], ring_sem.at[slot])]
        return [pltpu.make_async_copy(wd.at[layer, pl.ds(n_dn * CHUNK, dn_rest)], ring.at[slot, pl.ds(0, dn_rest)], ring_sem.at[slot])]

    def wait_chunk(kind, slot):
        place = ring.at[slot, pl.ds(0, dn_rest)] if kind == 'rest' else ring.at[slot]
        pltpu.make_async_copy(place, place, ring_sem.at[slot]).wait()

    def chunk_of(c):
        layer, r = divmod(c, per_layer)
        if r < at_gu:
            return 'wo', layer, r
        if r < at_dn:
            return 'gu', layer, r - at_gu
        if r < at_dn + n_dn:
            return 'dn', layer, r - at_dn
        return 'rest', layer, 0

    queue = []
    for layer in range(layers):
        queue += [('qkv', layer), ('cache', layer)]
        queue += [('chunk', c) for c in range(layer * per_layer, (layer + 1) * per_layer)]
    state = {'next': 0, 'under_way': 0, 'free_chunks': SLOTS, 'free_qkv': 1}
    size_of = {'qkv': QKV_CHUNKS, 'cache': CACHE_CHUNKS, 'chunk': 1}

    def started(*item):
        assert queue.index(item) < state['next'], item

    def fill(limit, stop=None):
        while state['next'] < len(queue) and queue[state['next']] != stop:
            kind, index = queue[state['next']]
            if state['under_way'] and state['under_way'] + size_of[kind] > limit:
                return
            if kind == 'qkv':
                if index >= state['free_qkv']:
                    return
                for j in range(QKV_PARTS):
                    for copy in qkv_copies(index, j):
                        copy.start()
            elif kind == 'cache':
                for copy in cache_copies(index):
                    copy.start()
            else:
                if index >= state['free_chunks']:
                    return
                for copy in chunk_copies(*chunk_of(index), index % SLOTS):
                    copy.start()
            state['under_way'] += size_of[kind]
            state['next'] += 1

    def stream_dot(lhs_ref, layer, first, groups):
        out = jnp.zeros(acc.shape, F32)
        row = 0
        c = layer * per_layer + first
        for group in groups:
            members = range(c, c + group)
            for i in members:
                started('chunk', i)
                wait_chunk(chunk_of(i)[0], i % SLOTS)
            state['under_way'] -= group
            fill(WINDOW)
            for i in members:
                n = dn_rest if chunk_of(i)[0] == 'rest' else CHUNK
                out = out + jnp.dot(lhs_ref[:, pl.ds(row, n)], ring[i % SLOTS, pl.ds(0, n)], preferred_element_type=F32)
                row += n
            state['free_chunks'] += group
            c += group
        acc[...] = out
        fill(WINDOW)

    def stream_loop(lhs_ref, layer, first, kind, steps, group, in_loop):
        base = layer * per_layer + first
        acc[...] = jnp.zeros_like(acc)
        ahead = 0
        if state['next'] < len(queue) and queue[state['next']] == ('chunk', base + steps * group):
            ahead = min(in_loop, n_dn // steps)
        for _ in range(ahead * steps):
            assert chunk_of(queue[state['next']][1])[0] == 'dn' and queue[state['next']][1] < base + SLOTS
            state['next'] += 1
            state['under_way'] += 1

        started('chunk', base + steps * group - 1)

        def body(i, carry):
            members = [(i * group + j, rem(base + i * group + j, SLOTS)) for j in range(group)]
            for k, slot in members:
                wait_chunk(kind, slot)
            for j in range(ahead):
                for copy in chunk_copies('dn', layer, i * ahead + j, rem(base + steps * group + i * ahead + j, SLOTS)):
                    copy.start()
            out = acc[...]
            for k, slot in members:
                lhs = lhs_ref[:, pl.ds(pl.multiple_of(k * CHUNK, CHUNK), CHUNK)]
                out = out + jnp.dot(lhs, ring[slot], preferred_element_type=F32)
            acc[...] = out
            return carry

        lax.fori_loop(0, steps, body, 0)
        state['under_way'] -= steps * group
        state['free_chunks'] += steps * group
        fill(WINDOW)

    qkv_rows = width // QKV_PARTS

    def qkv_copies(layer, j):
        piece = pl.ds(j * qkv_rows, qkv_rows)
        return [pltpu.make_async_copy(src.at[layer, piece], dst.at[piece], qkv_sem.at[i, j])
                for i, (src, dst) in enumerate(((wq, bq), (wk, bk), (wv, bv)))]

    def cache_copies(layer):
        pairs = ((kl_in, kl), (vl_in, vl)) if layer == 0 else ((kg_in, kg), (vg_in, vg))
        return [pltpu.make_async_copy(src, dst, cache_sem.at[layer, i]) for i, (src, dst) in enumerate(pairs)]

    def send_copies(phase):
        copies = []
        for step in far_first(n_tp):
            peer = lax.rem(me + step, n_tp)
            copies.append(pltpu.make_async_remote_copy(
                src_ref=part.at[phase, me], dst_ref=part.at[phase, me],
                send_sem=send_sem.at[phase], recv_sem=recv_sem.at[phase],
                device_id={'tp': peer}, device_id_type=MESH))
        return copies

    def all_copies(phase):
        blocks = part.at[phase, pl.ds(0, n_tp - 1)]
        return pltpu.make_async_remote_copy(
            src_ref=blocks, dst_ref=blocks, send_sem=send_sem.at[phase], recv_sem=recv_sem.at[phase],
            device_id={'tp': me}, device_id_type=MESH)

    def exchange(phase, limit, stop=None, meanwhile=None):
        part[phase, me] = acc[...].astype(BF16)
        copies = send_copies(phase)
        for copy in copies:
            copy.start()
        fill(limit, stop)
        if meanwhile is not None:
            meanwhile()
        all_copies(phase).wait_recv()
        total = part[phase, 0].astype(F32)
        for j in range(1, n_tp):
            total = total + part[phase, j].astype(F32)
        return total

    def gain(layer, i):
        return norm_ref[layer, pl.ds(i, 1), :]

    def add_normed(layer, i, branch_sum):
        x = (x_ref[...] + rms_norm(branch_sum, gain(layer, i)).astype(F32)).astype(BF16)
        x_ref[...] = x.astype(F32)
        return x

    def rotate(values, trig):
        first, second = values[:, :half], values[:, half:]
        cos_part, sin_part = trig
        return jnp.concatenate([first * cos_part - second * sin_part, second * cos_part + first * sin_part], axis=-1)

    def store_row(cache, b, slot, new_row):
        n = cache.shape[1]
        step = min(n, KV_STEP)

        def body(i, carry):
            piece = pl.ds(pl.multiple_of(i * step, step), step)
            ids = lax.broadcasted_iota(jnp.int32, (step, head), 0) + i * step
            cache[b, piece] = jnp.where(ids == slot, jnp.broadcast_to(new_row, (step, head)), cache[b, piece])
            return carry

        lax.fori_loop(0, n // step, body, 0)

    def attention(layer, kc, vc, trig):
        n = kc.shape[1]
        a_ref[...] = rms_norm(x_ref[...], gain(layer, 0))
        hq = bq.shape[1]

        started('qkv', layer)

        def qkv_body(j, carry):
            q, k, v = carry
            for copy in qkv_copies(layer, j):
                copy.wait()
            piece = pl.ds(pl.multiple_of(j * qkv_rows, qkv_rows), qkv_rows)
            lhs = a_ref[:, piece]
            q = q + jnp.dot(lhs, bq[piece], preferred_element_type=F32)
            k = k + jnp.dot(lhs, bk[piece], preferred_element_type=F32)
            v = v + jnp.dot(lhs, bv[piece], preferred_element_type=F32)
            return q, k, v

        q, k, v = lax.fori_loop(0, QKV_PARTS, qkv_body, (
            jnp.zeros((rows, hq), F32), jnp.zeros((rows, head), F32), jnp.zeros((rows, head), F32)))
        state['under_way'] -= QKV_CHUNKS
        state['free_qkv'] += 1
        fill(WINDOW)
        group = hq // head
        queries = jnp.concatenate([rotate(q[:, g * head:(g + 1) * head], trig) for g in range(group)], axis=0).astype(BF16)
        k_new = rotate(k, trig).astype(BF16)
        v_new = v.astype(BF16)
        started('cache', layer)
        for copy in cache_copies(layer):
            copy.wait()
        state['under_way'] -= CACHE_CHUNKS
        fill(WINDOW)
        q_rows = group * rows
        row_seq = lax.rem(lax.broadcasted_iota(jnp.int32, (q_rows, 1), 0), rows)
        last, slot = jnp.zeros((q_rows, 1), jnp.int32), jnp.zeros((q_rows, 1), jnp.int32)
        for b in range(rows):
            last = jnp.where(row_seq == b, pos_ref[b], last)
            slot = jnp.where(row_seq == b, lax.rem(pos_ref[b], n), slot)

        def pick(per_seq):
            out = per_seq[0]
            for b in range(1, rows):
                out = jnp.where(row_seq == b, per_seq[b], out)
            return out

        step = min(n, KV_STEP)
        contract_last = (((1,), (1,)), ((), ()))

        def soft_exp(s):
            return jnp.exp(SOFT_CAP * jnp.tanh(s * (head ** -0.5 / SOFT_CAP)))

        per_row = [jnp.concatenate([new.astype(F32)] * group, axis=0) for new in (k_new, v_new)]
        e_new = soft_exp(jnp.sum(queries.astype(F32) * per_row[0], axis=-1, keepdims=True))
        total = e_new
        def score_body(i, total):
            piece = pl.ds(pl.multiple_of(i * step, step), step)
            s = pick([lax.dot_general(queries, kc[b, piece], contract_last, preferred_element_type=F32) for b in range(rows)])
            ids = lax.broadcasted_iota(jnp.int32, (q_rows, step), 1) + i * step
            e = jnp.where((ids <= last) & (ids != slot), soft_exp(s), 0.0)
            e_ref[:, piece] = e
            return total + jnp.sum(e, axis=-1, keepdims=True)

        total = lax.fori_loop(0, n // step, score_body, total)

        def value_body(i, out):
            piece = pl.ds(pl.multiple_of(i * step, step), step)
            probs = (e_ref[:, piece] * inv_total).astype(BF16)
            return out + pick([jnp.dot(probs, vc[b, piece], preferred_element_type=F32) for b in range(rows)])

        inv_total = 1.0 / total
        out = (e_new * inv_total).astype(BF16).astype(F32) * per_row[1]
        out = lax.fori_loop(0, n // step, value_body, out)
        mixed = out.astype(BF16)
        for g in range(group):
            o_ref[:, pl.ds(g * head, head)] = mixed[g * rows:(g + 1) * rows]

        def store_new():
            for b in range(rows):
                store_row(kc, b, lax.rem(pos_ref[b], n), k_new[b:b + 1])
                store_row(vc, b, lax.rem(pos_ref[b], n), v_new[b:b + 1])

        return store_new

    small = [pltpu.make_async_copy(src, dst, small_sem.at[i]) for i, (src, dst) in enumerate(
        ((hid_in, hid_ref), (norm_in, norm_ref), (pos_in, pos_ref), (freq_in, freq_ref)))]
    for copy in small:
        copy.start()
    fill(START_WINDOW)

    barrier = pltpu.get_barrier_semaphore()
    for step in range(1, n_tp):
        pl.semaphore_signal(barrier, inc=1, device_id={'tp': lax.rem(me + step, n_tp)}, device_id_type=MESH)

    for copy in small:
        copy.wait()
    x_ref[...] = hid_ref[...].astype(F32)
    row_ids = lax.broadcasted_iota(jnp.int32, (rows, half), 0)
    pos_rows = jnp.zeros((rows, half), F32)
    for b in range(rows):
        pos_rows = jnp.where(row_ids == b, pos_ref[b].astype(F32), pos_rows)
    angles = pos_rows * freq_ref[...]
    trig = jnp.cos(angles), jnp.sin(angles)
    for layer in range(layers):
        kc, vc = (kl, vl) if layer == 0 else (kg, vg)
        store_new = attention(layer, kc, vc, trig)
        stream_dot(o_ref, layer, 0, (n_wo,))
        if layer == 0:
            pl.semaphore_wait(barrier, n_tp - 1)
        x = add_normed(layer, 1, exchange(2 * layer, len(queue) * QKV_CHUNKS, ('chunk', at_dn), store_new))
        a_ref[...] = rms_norm(x.astype(F32), gain(layer, 2))
        stream_loop(a_ref, layer, at_gu, 'gu', n_gu // GU_GROUP, GU_GROUP, 2)
        gate_up = acc[...]
        h_ref[...] = (jax.nn.gelu(gate_up[:, :ff], approximate=True) * gate_up[:, ff:]).astype(BF16)
        stream_dot(h_ref, layer, at_dn, split(per_layer - at_dn, DN_GROUP if layer == 0 else LATE_DN_GROUP))
        x = add_normed(layer, 3, exchange(2 * layer + 1, SUM_WINDOW))
    hid_out[...] = x
    for phase in range(2 * layers):
        all_copies(phase).wait_send()


def write_kernel(*refs):
    n = len(refs) // 2
    for i in range(n):
        for b in range(refs[i].shape[0] if len(refs[i].shape) > 2 else 1):
            part = refs[i].at[b] if len(refs[i].shape) > 2 else refs[i]
            place = refs[n + i].at[b] if len(refs[i].shape) > 2 else refs[n + i]
            pltpu.make_async_copy(part, place, refs[-1].at[i]).start()
    for i in range(n):
        pltpu.make_async_copy(refs[i], refs[n + i], refs[-1].at[i]).wait()


def decode_step(n_tp, hidden, positions, k_local, v_local, k_global, v_global, w_query, w_key, w_value, w_out, w_gate, w_up, w_down, norm_scale):
    rows, width = hidden.shape
    caches = [c.reshape(c.shape[0], c.shape[1], c.shape[3]) for c in (k_local, v_local, k_global, v_global)]
    head = caches[0].shape[2]
    half = head // 2
    inv_freq = jnp.asarray(ROPE_BASE ** (-2.0 * np.arange(half) / head), F32)[None, :]
    hq, ff, layers = w_query.shape[2], w_gate.shape[2], w_gate.shape[0]
    n_ctx = max(c.shape[1] for c in caches)
    vmem = pl.BlockSpec(memory_space=pltpu.VMEM)
    hbm = pl.BlockSpec(memory_space=pl.ANY)
    outs = pl.pallas_call(
        functools.partial(step_kernel, n_tp),
        out_shape=tuple(pltpu.VMEM(a.shape, BF16) for a in (hidden, *caches)),
        in_specs=[hbm] * 15,
        out_specs=(vmem,) * 5,
        scratch_shapes=[
            pltpu.SMEM((rows,), jnp.int32),
            pltpu.VMEM((rows, width), BF16),
            pltpu.VMEM((1, half), F32),
            pltpu.VMEM(norm_scale.shape, F32),
            pltpu.VMEM((SLOTS, CHUNK, width), BF16),
            pltpu.VMEM((width, hq), BF16),
            pltpu.VMEM((width, head), BF16),
            pltpu.VMEM((width, head), BF16),
            pltpu.VMEM((rows, width), F32),
            pltpu.VMEM((rows, width), BF16),
            pltpu.VMEM((rows, hq), BF16),
            pltpu.VMEM((rows, ff), BF16),
            pltpu.VMEM((rows, 2 * ff), F32),
            pltpu.VMEM((hq // head * rows, n_ctx), F32),
            pltpu.VMEM((2 * layers, n_tp, rows, width), BF16),
            pltpu.SemaphoreType.DMA((4,)),
            pltpu.SemaphoreType.DMA((SLOTS,)),
            pltpu.SemaphoreType.DMA((3, QKV_PARTS)),
            pltpu.SemaphoreType.DMA((2, 2)),
            pltpu.SemaphoreType.DMA((2 * layers,)),
            pltpu.SemaphoreType.DMA((2 * layers,)),
        ],
        compiler_params=pltpu.CompilerParams(
            collective_id=0, has_side_effects=True, vmem_limit_bytes=VMEM_LIMIT),
        name='decode_step',
    )(positions, hidden, inv_freq, norm_scale, *caches, w_query, w_key, w_value, w_out, w_gate, w_up, w_down)
    hidden_out, *new_caches = pl.pallas_call(
        write_kernel,
        out_shape=tuple(jax.ShapeDtypeStruct(o.shape, o.dtype) for o in outs),
        in_specs=[hbm] * len(outs),
        out_specs=(hbm,) * len(outs),
        scratch_shapes=[pltpu.SemaphoreType.DMA((len(outs),))],
        compiler_params=pltpu.CompilerParams(vmem_limit_bytes=1024 * 1024),
        name='write_out',
    )(*outs)
    new_caches = [c.reshape(old.shape) for c, old in zip(new_caches, (k_local, v_local, k_global, v_global))]
    return (hidden_out, *new_caches)


def solution(mesh):
    row_spec = P('dp', None)
    cache_spec = P('dp', None, 'tp', None)
    col_split = P(None, None, 'tp')
    row_split = P(None, 'tp', None)
    in_specs = (row_spec, P('dp'), cache_spec, cache_spec, cache_spec, cache_spec, col_split, col_split, col_split, row_split, col_split, col_split, row_split, P())
    out_specs = (row_spec, cache_spec, cache_spec, cache_spec, cache_spec)
    return jax.shard_map(functools.partial(decode_step, mesh.shape['tp']), mesh=mesh, in_specs=in_specs, out_specs=out_specs, check_vma=False)
```
